16 devices in a mesh: rep: 1, dp: 16 (over x, y, z, core).
Axes of the slice: x: 2, y: 2, z: 2, core: 2. Of those that a mesh axis runs over, the one named last changes fastest.
Arguments:
- g_w_gate: bfloat16 [16, 2, 512, 8192], P(('rep', 'dp'))
- g_w_up: bfloat16 [16, 2, 512, 8192], P(('rep', 'dp'))
- g_w_down: bfloat16 [16, 2, 8192, 512], P(('rep', 'dp'))
- w_gate: bfloat16 [2, 512, 8192], replicated
- w_up: bfloat16 [2, 512, 8192], replicated
- w_down: bfloat16 [2, 8192, 512], replicated
- m_w_gate: float32 [2, 512, 8192], P(None, 'dp')
- m_w_up: float32 [2, 512, 8192], P(None, 'dp')
- m_w_down: float32 [2, 8192, 512], P(None, 'dp')
- v_w_gate: float32 [2, 512, 8192], P(None, 'dp')
- v_w_up: float32 [2, 512, 8192], P(None, 'dp')
- v_w_down: float32 [2, 8192, 512], P(None, 'dp')
Outputs:
- output 1: bfloat16 [2, 512, 8192], P('rep')
- output 2: bfloat16 [2, 512, 8192], P('rep')
- output 3: bfloat16 [2, 8192, 512], P('rep')
- output 4: float32 [2, 512, 8192], P('rep', 'dp')
- output 5: float32 [2, 512, 8192], P('rep', 'dp')
- output 6: float32 [2, 8192, 512], P('rep', 'dp')
- output 7: float32 [2, 512, 8192], P('rep', 'dp')
- output 8: float32 [2, 512, 8192], P('rep', 'dp')
- output 9: float32 [2, 8192, 512], P('rep', 'dp')
All inputs are finite; a program needn't handle non-finite values.
Results may differ from the reference program's by a relative error of at most 0.022.
Values are sent between devices in bfloat16 or wider.
A program may use at most 2 GiB of HBM per device.

```python
import jax
import jax.numpy as jnp
from jax import lax

DEVICES = 16
D = 512
FF = 8192
LAYERS = 2
NAMES = ("w_gate", "w_up", "w_down")
SHAPES = {"w_gate": (LAYERS, D, FF), "w_up": (LAYERS, D, FF), "w_down": (LAYERS, FF, D)}


def setup_inputs(seed: int = 0, part: int = 0) -> dict:
    kz, *keys = jax.random.split(jax.random.key(seed), 1 + 5 * len(NAMES))
    loud = 2.0 ** jax.random.uniform(kz, (), jnp.float32, -1.0, 1.0)
    drawn = {}
    for name, key, both in zip(NAMES, keys[:3], keys[3:6], strict=True):
        own = jax.random.normal(jax.random.fold_in(key, part), (DEVICES, *SHAPES[name]), jnp.float32)
        shared = jax.random.normal(jax.random.fold_in(both, part), SHAPES[name], jnp.float32)
        drawn["g_" + name] = (loud * (0.7 * shared / DEVICES + 0.7 * own * DEVICES**-0.5)).astype(jnp.bfloat16)
    for name, key in zip(NAMES, keys[6:9], strict=True):
        drawn[name] = (jax.random.normal(key, SHAPES[name], jnp.float32) * SHAPES[name][1] ** -0.5).astype(jnp.bfloat16)
    for name, key in zip(NAMES, keys[9:12], strict=True):
        drawn["m_" + name] = loud * 0.5 * jax.random.normal(key, SHAPES[name], jnp.float32)
    for name, key in zip(NAMES, keys[12:15], strict=True):
        drawn["v_" + name] = loud * loud * jax.random.uniform(key, SHAPES[name], jnp.float32, 0.5, 1.5)
    return drawn


def adamw(w, m, v, g):
    m = 0.9 * m + 0.1 * g
    v = 0.95 * v + 0.05 * g * g
    step = m * lax.rsqrt(v + 1e-8) + 0.1 * w
    return (w - 0.02 * step).astype(jnp.bfloat16), m, v


def reference(g_w_gate, g_w_up, g_w_down, w_gate, w_up, w_down, m_w_gate, m_w_up, m_w_down, v_w_gate, v_w_up, v_w_down):
    def total(terms):
        return lax.scan(lambda so_far, term: (so_far + term.astype(jnp.float32), None), jnp.zeros(terms.shape[1:], jnp.float32), terms)[0]

    gradients = [total(terms).astype(jnp.bfloat16).astype(jnp.float32) for terms in (g_w_gate, g_w_up, g_w_down)]
    new = [
        adamw(w.astype(jnp.float32), m, v, g)
        for w, m, v, g in zip((w_gate, w_up, w_down), (m_w_gate, m_w_up, m_w_down), (v_w_gate, v_w_up, v_w_down), gradients, strict=True)
    ]
    return tuple(one[which] for which in range(3) for one in new)
```

```python
import functools

import jax
import jax.numpy as jnp
from jax import lax
from jax.experimental import pallas as pl
from jax.experimental.pallas import tpu as pltpu
from jax.sharding import PartitionSpec as P

SUB = 4
LAYERS = 2
J = LAYERS * SUB
AHEAD = 2
STRIDE = {"x": 8, "y": 4, "z": 2}
ORDER = (("x", "y", "z"), ("y", "z", "x"), ("z", "x", "y"))
C = 3
F32, BF16 = jnp.float32, jnp.bfloat16
MESH = pl.DeviceIdType.MESH
D0, S1, S2, S3, A1, A2, A3, FW = range(8)


def adamw(w, m, v, g):
    m = 0.9 * m + 0.1 * g
    v = 0.95 * v + 0.05 * g * g
    step = m * lax.rsqrt(v + 1e-8) + 0.1 * w
    return (w - 0.02 * step).astype(BF16), m, v


def kernel(*refs):
    it = iter(refs)

    def take(n=C):
        return [next(it) for _ in range(n)]

    g, w, m, v = take(), take(), take(), take()
    out, m_out, v_out = take(), take(), take()
    r0, r1, r2, r3 = take(), take(), take(), take()
    o1, o2, o3, o4 = take(), take(), take(), take()
    mb, vb, wb = take(), take(), take()
    send, recv, local, load, moved = take(5)

    me = lax.axis_index("dp")
    core = me % 2
    bit = {d: me // s % 2 for d, s in STRIDE.items()}
    near = {d: me + s * (1 - 2 * bit[d]) for d, s in STRIDE.items()}
    partner = me + 1 - 2 * core
    mine = [tuple(bit[d] for d in ORDER[c]) for c in range(C)]

    def block(c, b0, b1, b2, k):
        s = [STRIDE[d] for d in ORDER[c]]
        return b0 * s[0] + b1 * s[1] + b2 * s[2] + k

    def part(c, j):
        layer, s = j // SUB, j % SUB
        if c < 2:
            width = 8192 // SUB
            return layer, slice(None), pl.ds(pl.multiple_of(s * width, width), width)
        height = 512 // SUB
        return layer, pl.ds(pl.multiple_of(s * height, height), height), slice(None)

    def of_block(ref, c, blk, j):
        layer, rows, columns = part(c, j)
        return ref.at[layer, blk, rows, columns]

    def of_own(ref, c, j):
        layer, rows, columns = part(c, j)
        return ref.at[layer, rows, columns]

    def remote(c, j, group, src, dst, to):
        return pltpu.make_async_remote_copy(
            src_ref=src, dst_ref=dst, send_sem=send.at[group, c, j], recv_sem=recv.at[group, c, j], device_id={"dp": to}, device_id_type=MESH
        )

    def wait_for(ref, sem):
        pltpu.make_async_copy(ref, ref, sem).wait()

    def tiles(c, body, rows=32):
        if c < 2:
            across, down, high = 8192 // SUB // 512, 32 // rows, rows
        else:
            across, down = 1, 512 // SUB // rows

        @pl.loop(0, across * down)
        def _(i):
            row = pl.multiple_of(i % down * rows, rows)
            column = pl.multiple_of(i // down * 512, 512)
            body((pl.ds(row, rows), pl.ds(column, 512)))

    def start_exchange(j):
        for c in range(C):
            for p in range(8):
                blk = block(c, p // 4, p // 2 % 2, p % 2, 1 - core)
                remote(c, j, D0, of_block(g[c], c, blk, j), r0[c].at[j, p], partner).start()

    def load_terms(stage, j):
        slot = j % 2
        for c in range(C):
            m0, m1, m2 = mine[c]
            if stage == 0:
                places = [(1 - m0, q // 2, q % 2) for q in range(4)]
            elif stage == 1:
                places = [(m0, 1 - m1, q) for q in range(2)]
            elif stage == 2:
                places = [(m0, m1, 1 - m2)]
            else:
                places = [(m0, m1, m2)]
            to = (o1, o2, o3, o4)[stage][c]
            for q, place in enumerate(places):
                pltpu.make_async_copy(of_block(g[c], c, block(c, *place, core), j), to.at[slot, q], load.at[stage, c, slot]).start()

    def load_own(j):
        slot = j % 2
        for c in range(C):

            @pl.when(j >= 2)
            def _():
                wait_for(mb[c].at[slot], moved.at[0, c, slot])
                wait_for(vb[c].at[slot], moved.at[1, c, slot])

            pltpu.make_async_copy(of_own(m[c], c, j), mb[c].at[slot], load.at[4, c, slot]).start()
            pltpu.make_async_copy(of_own(v[c], c, j), vb[c].at[slot], load.at[5, c, slot]).start()
            pltpu.make_async_copy(of_block(w[c], c, me, j), wb[c].at[slot], load.at[6, c, slot]).start()

    def stage1(j):
        slot = j % 2
        for c in range(C):
            m0, m1, m2 = mine[c]
            wait_for(r0[c].at[j], recv.at[D0, c, j])
            wait_for(o1[c].at[slot], load.at[0, c, slot])

            def body(at):
                for q in range(4):
                    p = (1 - m0) * 4 + q
                    r0[c][(j, p, *at)] = (r0[c][(j, p, *at)].astype(F32) + o1[c][(slot, q, *at)].astype(F32)).astype(BF16)

            tiles(c, body)
            remote(c, j, S1, r0[c].at[j, pl.ds((1 - m0) * 4, 4)], r1[c].at[j], near[ORDER[c][0]]).start()

    def stage2(j):
        slot = j % 2
        for c in range(C):
            m0, m1, m2 = mine[c]
            wait_for(o2[c].at[slot], load.at[1, c, slot])
            wait_for(r1[c].at[j], recv.at[S1, c, j])
            wait_for(r1[c].at[j], send.at[S1, c, j])

            def body(at):
                for q in range(2):
                    p = (1 - m1) * 2 + q
                    total = r0[c][(j, m0 * 4 + p, *at)].astype(F32) + o2[c][(slot, q, *at)].astype(F32)
                    r1[c][(j, p, *at)] = (total + r1[c][(j, p, *at)].astype(F32)).astype(BF16)

            tiles(c, body)
            remote(c, j, S2, r1[c].at[j, pl.ds((1 - m1) * 2, 2)], r2[c].at[j], near[ORDER[c][1]]).start()

    def stage3(j):
        slot = j % 2
        for c in range(C):
            m0, m1, m2 = mine[c]
            wait_for(o3[c].at[slot], load.at[2, c, slot])
            wait_for(r2[c].at[j], recv.at[S2, c, j])
            wait_for(r2[c].at[j], send.at[S2, c, j])

            def body(at):
                p = 1 - m2
                total = r0[c][(j, m0 * 4 + m1 * 2 + p, *at)].astype(F32) + o3[c][(slot, 0, *at)].astype(F32)
                total = total + r1[c][(j, m1 * 2 + p, *at)].astype(F32)
                r2[c][(j, p, *at)] = (total + r2[c][(j, p, *at)].astype(F32)).astype(BF16)

            tiles(c, body)
            remote(c, j, S3, r2[c].at[j, pl.ds(1 - m2, 1)], r3[c].at[j], near[ORDER[c][2]]).start()

    def give(c, j, p, n):
        for q in range(n):
            at = p + q
            to = of_block(out[c], c, block(c, at // 4, at // 2 % 2, at % 2, core), j)
            remote(c, j, FW, r0[c].at[j, at], to, partner).start()
            pltpu.make_async_copy(r0[c].at[j, at], to, local.at[c, j]).start()

    def stage4(j):
        slot = j % 2
        for c in range(C):
            m0, m1, m2 = mine[c]
            here = m0 * 4 + m1 * 2 + m2
            wait_for(o4[c].at[slot], load.at[3, c, slot])
            wait_for(mb[c].at[slot], load.at[4, c, slot])
            wait_for(vb[c].at[slot], load.at[5, c, slot])
            wait_for(wb[c].at[slot], load.at[6, c, slot])
            wait_for(r3[c].at[j], recv.at[S3, c, j])
            wait_for(r3[c].at[j], send.at[S3, c, j])

            def body(at):
                total = r0[c][(j, here, *at)].astype(F32) + o4[c][(slot, 0, *at)].astype(F32)
                total = total + r1[c][(j, m1 * 2 + m2, *at)].astype(F32)
                total = total + r2[c][(j, m2, *at)].astype(F32)
                total = total + r3[c][(j, 0, *at)].astype(F32)
                grad = total.astype(BF16).astype(F32)
                new = adamw(wb[c][(slot, *at)].astype(F32), mb[c][(slot, *at)], vb[c][(slot, *at)], grad)
                r0[c][(j, here, *at)], mb[c][(slot, *at)], vb[c][(slot, *at)] = new

            tiles(c, body, rows=16)
            remote(c, j, A1, r0[c].at[j, here], r0[c].at[j, here], near[ORDER[c][2]]).start()
            pltpu.make_async_copy(mb[c].at[slot], of_own(m_out[c], c, j), moved.at[0, c, slot]).start()
            pltpu.make_async_copy(vb[c].at[slot], of_own(v_out[c], c, j), moved.at[1, c, slot]).start()
            give(c, j, here, 1)

    def stage5(j):
        for c in range(C):
            m0, m1, m2 = mine[c]
            pair = m0 * 4 + m1 * 2
            wait_for(r3[c].at[j], recv.at[A1, c, j])
            remote(c, j, A2, r0[c].at[j, pl.ds(pair, 2)], r0[c].at[j, pl.ds(pair, 2)], near[ORDER[c][1]]).start()
            give(c, j, pair + 1 - m2, 1)

    def stage6(j):
        for c in range(C):
            m0, m1, m2 = mine[c]
            wait_for(r2[c].at[j], recv.at[A2, c, j])
            remote(c, j, A3, r0[c].at[j, pl.ds(m0 * 4, 4)], r0[c].at[j, pl.ds(m0 * 4, 4)], near[ORDER[c][0]]).start()
            give(c, j, m0 * 4 + (1 - m1) * 2, 2)

    def stage7(j):
        for c in range(C):
            m0, m1, m2 = mine[c]
            wait_for(r1[c].at[j], recv.at[A3, c, j])
            give(c, j, (1 - m0) * 4, 4)

    barrier = pltpu.get_barrier_semaphore()
    for to in (partner, *near.values()):
        pl.semaphore_signal(barrier, inc=1, device_id={"dp": to}, device_id_type=MESH)
    pl.semaphore_wait(barrier, 4)

    for j in range(AHEAD):
        start_exchange(j)
    load_terms(0, 0)

    @pl.loop(0, J + 6)
    def _(t):
        def on(j, run):
            pl.when(jnp.logical_and(j >= 0, j < J))(lambda: run(j))

        on(t + AHEAD, start_exchange)
        on(t + 1, functools.partial(load_terms, 0))
        on(t, functools.partial(load_terms, 1))
        on(t - 1, functools.partial(load_terms, 2))
        on(t - 2, functools.partial(load_terms, 3))
        on(t - 2, load_own)
        for back, stage in enumerate((stage1, stage2, stage3, stage4, stage5, stage6, stage7)):
            on(t - back, stage)

    for c in range(C):
        for slot in range(2):
            wait_for(mb[c].at[slot], moved.at[0, c, slot])
            wait_for(vb[c].at[slot], moved.at[1, c, slot])

    @pl.loop(0, J)
    def _(j):
        for c in range(C):
            wait_for(r0[c].at[j], send.at[D0, c, j])
            wait_for(r3[c].at[j], send.at[A1, c, j])
            wait_for(r2[c].at[j], send.at[A2, c, j])
            wait_for(r1[c].at[j], send.at[A3, c, j])
            wait_for(r0[c].at[j], local.at[c, j])
            wait_for(r0[c].at[j], send.at[FW, c, j])
            wait_for(r0[c].at[j], recv.at[FW, c, j])


def solution(mesh):
    chunk = ((32, 8192 // SUB),) * 2 + ((512 // SUB, 512),)
    blocks = ((LAYERS, 16, 32, 8192),) * 2 + ((LAYERS, 16, 512, 512),)
    own = ((LAYERS, 32, 8192),) * 2 + ((LAYERS, 512, 512),)
    whole = ((LAYERS, 512, 8192),) * 2 + ((LAYERS, 8192, 512),)

    def vmem(*lead, dtype=BF16):
        return [pltpu.VMEM((*lead, *chunk[c]), dtype) for c in range(C)]

    call = pl.pallas_call(
        kernel,
        out_shape=[jax.ShapeDtypeStruct(s, BF16) for s in blocks] + [jax.ShapeDtypeStruct(s, F32) for s in own] * 2,
        in_specs=[pl.BlockSpec(memory_space=pl.ANY)] * 12,
        out_specs=[pl.BlockSpec(memory_space=pl.ANY)] * 9,
        scratch_shapes=[
            *vmem(J, 8),
            *vmem(J, 4),
            *vmem(J, 2),
            *vmem(J, 1),
            *vmem(2, 4),
            *vmem(2, 2),
            *vmem(2, 1),
            *vmem(2, 1),
            *vmem(2, dtype=F32),
            *vmem(2, dtype=F32),
            *vmem(2),
            pltpu.SemaphoreType.DMA((8, C, J)),
            pltpu.SemaphoreType.DMA((8, C, J)),
            pltpu.SemaphoreType.DMA((C, J)),
            pltpu.SemaphoreType.DMA((7, C, 2)),
            pltpu.SemaphoreType.DMA((2, C, 2)),
        ],
        compiler_params=pltpu.CompilerParams(collective_id=0, has_side_effects=True, vmem_limit_bytes=67043328),
    )

    def step(*arrays):
        terms = [a.reshape(s) for a, s in zip(arrays[:3], blocks, strict=True)]
        weights = [a.reshape(s) for a, s in zip(arrays[3:6], blocks, strict=True)]
        new = call(*terms, *weights, *arrays[6:])
        return (*(a.reshape(s) for a, s in zip(new[:3], whole, strict=True)), *new[3:])

    all_of, cut = P(None, None, None), P(None, "dp", None)
    return jax.shard_map(
        step,
        mesh=mesh,
        in_specs=(P(("rep", "dp"), None, None, None),) * 3 + (all_of,) * 3 + (cut,) * 6,
        out_specs=(P("rep", None, None),) * 3 + (P("rep", "dp", None),) * 6,
        check_vma=False,
    )
```

```python
import functools

import jax
import jax.numpy as jnp
from jax import lax
from jax.experimental import pallas as pl
from jax.experimental.pallas import tpu as pltpu
from jax.sharding import PartitionSpec as P

SUB = 8
LAYERS = 2
J = LAYERS * SUB
RING = 6
AHEAD = 2
STRIDE = {"x": 8, "y": 4, "z": 2}
ORDER = (("x", "y", "z"), ("y", "z", "x"), ("z", "x", "y"))
C = 3
F32, BF16 = jnp.float32, jnp.bfloat16
MESH = pl.DeviceIdType.MESH
D0, DN, S1, S2, S3, A1, A2, A3, FW = range(9)


def adamw(w, m, v, g):
    m = 0.9 * m + 0.1 * g
    v = 0.95 * v + 0.05 * g * g
    step = m * lax.rsqrt(v + 1e-8) + 0.1 * w
    return (w - 0.02 * step).astype(BF16), m, v


def place(c, b0, b1, b2, k):
    s = [STRIDE[d] for d in ORDER[c]]
    return b0 * s[0] + b1 * s[1] + b2 * s[2] + k


def part(c, j):
    layer, s = j // SUB, j % SUB
    if c < 2:
        width = 8192 // SUB
        return layer, slice(None), pl.ds(pl.multiple_of(s * width, width), width)
    height = 512 // SUB
    return layer, pl.ds(pl.multiple_of(s * height, height), height), slice(None)


def kernel(*refs):
    it = iter(refs)

    def take(n=C):
        return [next(it) for _ in range(n)]

    g, w, m, v = take(), take(), take(), take()
    r0, other, m_out, v_out = take(), take(), take(), take()
    r1, r2, r3 = take(), take(), take()
    o1, o2, o3, o4 = take(), take(), take(), take()
    mb, vb, wb = take(), take(), take()
    send, recv, load, moved = take(4)

    me = lax.axis_index("dp")
    core = me % 2
    bit = {d: me // s % 2 for d, s in STRIDE.items()}
    near = {d: me + s * (1 - 2 * bit[d]) for d, s in STRIDE.items()}
    partner = me + 1 - 2 * core
    mine = [tuple(bit[d] for d in ORDER[c]) for c in range(C)]

    def of_block(ref, c, blk, j):
        layer, rows, columns = part(c, j)
        return ref.at[layer, blk, rows, columns]

    def of_own(ref, c, j):
        layer, rows, columns = part(c, j)
        return ref.at[layer, rows, columns]

    def remote(c, j, group, src, dst, to):
        return pltpu.make_async_remote_copy(
            src_ref=src, dst_ref=dst, send_sem=send.at[group, c, j], recv_sem=recv.at[group, c, j], device_id={"dp": to}, device_id_type=MESH
        )

    def wait_for(ref, sem):
        pltpu.make_async_copy(ref, ref, sem).wait()

    def tiles(c, body, rows=32):
        if c < 2:
            across, down, high = 8192 // SUB // 512, 32 // rows, rows
        else:
            across, down = 1, 512 // SUB // rows

        @pl.loop(0, across * down)
        def _(i):
            row = pl.multiple_of(i % down * rows, rows)
            column = pl.multiple_of(i // down * 512, 512)
            body((pl.ds(row, rows), pl.ds(column, 512)))

    def start_exchange(j):
        for group in (D0, DN):
            for c in range(C):
                half = 1 - mine[c][0] if group == D0 else mine[c][0]
                for q in range(4):
                    blk = place(c, half, q // 2, q % 2, 1 - core)
                    remote(c, j, group, of_block(g[c], c, blk, j), r0[c].at[j, half * 4 + q], partner).start()

    def load_terms(stage, j):
        slot = j % 2
        for c in range(C):
            m0, m1, m2 = mine[c]
            if stage == 0:
                places = [(1 - m0, q // 2, q % 2) for q in range(4)]
            elif stage == 1:
                places = [(m0, 1 - m1, q) for q in range(2)]
            elif stage == 2:
                places = [(m0, m1, 1 - m2)]
            else:
                places = [(m0, m1, m2)]
            to = (o1, o2, o3, o4)[stage][c]
            for q, bits in enumerate(places):
                pltpu.make_async_copy(of_block(g[c], c, place(c, *bits, core), j), to.at[slot, q], load.at[stage, c, slot]).start()

    def load_own(j):
        slot = j % 2
        for c in range(C):

            @pl.when(j >= 2)
            def _():
                wait_for(mb[c].at[slot], moved.at[0, c, slot])
                wait_for(vb[c].at[slot], moved.at[1, c, slot])

            pltpu.make_async_copy(of_own(m[c], c, j), mb[c].at[slot], load.at[4, c, slot]).start()
            pltpu.make_async_copy(of_own(v[c], c, j), vb[c].at[slot], load.at[5, c, slot]).start()
            pltpu.make_async_copy(of_block(w[c], c, me, j), wb[c].at[slot], load.at[6, c, slot]).start()

    def stage1(j):
        slot = j % 2
        for c in range(C):
            m0, m1, m2 = mine[c]
            wait_for(r1[c].at[0], recv.at[D0, c, j])
            wait_for(o1[c].at[slot], load.at[0, c, slot])

            def body(at):
                for q in range(4):
                    p = (1 - m0) * 4 + q
                    r0[c][(j, p, *at)] = (r0[c][(j, p, *at)].astype(F32) + o1[c][(slot, q, *at)].astype(F32)).astype(BF16)

            tiles(c, body)
            remote(c, j, S1, r0[c].at[j, pl.ds((1 - m0) * 4, 4)], r1[c].at[j % RING], near[ORDER[c][0]]).start()

    def stage2(j):
        slot, ring = j % 2, j % RING
        for c in range(C):
            m0, m1, m2 = mine[c]
            wait_for(o2[c].at[slot], load.at[1, c, slot])
            wait_for(r1[c].at[0], recv.at[DN, c, j])
            wait_for(r1[c].at[0], recv.at[S1, c, j])
            wait_for(r1[c].at[0], send.at[S1, c, j])

            def body(at):
                for q in range(2):
                    p = (1 - m1) * 2 + q
                    total = r0[c][(j, m0 * 4 + p, *at)].astype(F32) + o2[c][(slot, q, *at)].astype(F32)
                    r1[c][(ring, p, *at)] = (total + r1[c][(ring, p, *at)].astype(F32)).astype(BF16)

            tiles(c, body)
            remote(c, j, S2, r1[c].at[ring, pl.ds((1 - m1) * 2, 2)], r2[c].at[ring], near[ORDER[c][1]]).start()

    def stage3(j):
        slot, ring = j % 2, j % RING
        for c in range(C):
            m0, m1, m2 = mine[c]
            wait_for(o3[c].at[slot], load.at[2, c, slot])
            wait_for(r2[c].at[0], recv.at[S2, c, j])
            wait_for(r2[c].at[0], send.at[S2, c, j])

            def body(at):
                p = 1 - m2
                total = r0[c][(j, m0 * 4 + m1 * 2 + p, *at)].astype(F32) + o3[c][(slot, 0, *at)].astype(F32)
                total = total + r1[c][(ring, m1 * 2 + p, *at)].astype(F32)
                r2[c][(ring, p, *at)] = (total + r2[c][(ring, p, *at)].astype(F32)).astype(BF16)

            tiles(c, body)
            remote(c, j, S3, r2[c].at[ring, pl.ds(1 - m2, 1)], r3[c].at[ring], near[ORDER[c][2]]).start()

    def give(c, j, p, n):
        remote(c, j, FW, r0[c].at[j, pl.ds(p, n)], other[c].at[j, pl.ds(p, n)], partner).start()

    def stage4(j):
        slot, ring = j % 2, j % RING
        for c in range(C):
            m0, m1, m2 = mine[c]
            here = m0 * 4 + m1 * 2 + m2
            wait_for(o4[c].at[slot], load.at[3, c, slot])
            wait_for(mb[c].at[slot], load.at[4, c, slot])
            wait_for(vb[c].at[slot], load.at[5, c, slot])
            wait_for(wb[c].at[slot], load.at[6, c, slot])
            wait_for(r3[c].at[0], recv.at[S3, c, j])
            wait_for(r3[c].at[0], send.at[S3, c, j])

            def body(at):
                total = r0[c][(j, here, *at)].astype(F32) + o4[c][(slot, 0, *at)].astype(F32)
                total = total + r1[c][(ring, m1 * 2 + m2, *at)].astype(F32)
                total = total + r2[c][(ring, m2, *at)].astype(F32)
                total = total + r3[c][(ring, 0, *at)].astype(F32)
                grad = total.astype(BF16).astype(F32)
                new = adamw(wb[c][(slot, *at)].astype(F32), mb[c][(slot, *at)], vb[c][(slot, *at)], grad)
                r0[c][(j, here, *at)], mb[c][(slot, *at)], vb[c][(slot, *at)] = new

            tiles(c, body, rows=16)
            remote(c, j, A1, r0[c].at[j, here], r0[c].at[j, here], near[ORDER[c][2]]).start()
            pltpu.make_async_copy(mb[c].at[slot], of_own(m_out[c], c, j), moved.at[0, c, slot]).start()
            pltpu.make_async_copy(vb[c].at[slot], of_own(v_out[c], c, j), moved.at[1, c, slot]).start()
            give(c, j, here, 1)

    def stage5(j):
        for c in range(C):
            m0, m1, m2 = mine[c]
            pair = m0 * 4 + m1 * 2
            wait_for(r3[c].at[0], recv.at[A1, c, j])
            remote(c, j, A2, r0[c].at[j, pl.ds(pair, 2)], r0[c].at[j, pl.ds(pair, 2)], near[ORDER[c][1]]).start()
            give(c, j, pair + 1 - m2, 1)

    def stage6(j):
        for c in range(C):
            m0, m1, m2 = mine[c]
            wait_for(r2[c].at[0], recv.at[A2, c, j])
            remote(c, j, A3, r0[c].at[j, pl.ds(m0 * 4, 4)], r0[c].at[j, pl.ds(m0 * 4, 4)], near[ORDER[c][0]]).start()
            give(c, j, m0 * 4 + (1 - m1) * 2, 2)

    def stage7(j):
        for c in range(C):
            m0, m1, m2 = mine[c]
            wait_for(r1[c].at[0], recv.at[A3, c, j])
            give(c, j, (1 - m0) * 4, 4)

    barrier = pltpu.get_barrier_semaphore()
    for to in (partner, *near.values()):
        pl.semaphore_signal(barrier, inc=1, device_id={"dp": to}, device_id_type=MESH)
    pl.semaphore_wait(barrier, 4)

    for j in range(AHEAD):
        start_exchange(j)
    load_terms(0, 0)

    @pl.loop(0, J + 6)
    def _(t):
        def on(j, run):
            pl.when(jnp.logical_and(j >= 0, j < J))(lambda: run(j))

        on(t + AHEAD, start_exchange)
        on(t + 1, functools.partial(load_terms, 0))
        on(t, functools.partial(load_terms, 1))
        on(t - 1, functools.partial(load_terms, 2))
        on(t - 2, functools.partial(load_terms, 3))
        on(t - 2, load_own)
        for back, stage in enumerate((stage1, stage2, stage3, stage4, stage5, stage6, stage7)):
            on(t - back, stage)

    for c in range(C):
        for slot in range(2):
            wait_for(mb[c].at[slot], moved.at[0, c, slot])
            wait_for(vb[c].at[slot], moved.at[1, c, slot])

    @pl.loop(0, J)
    def _(j):
        for c in range(C):
            wait_for(r1[c].at[0], send.at[D0, c, j])
            wait_for(r1[c].at[0], send.at[DN, c, j])
            wait_for(r3[c].at[0], send.at[A1, c, j])
            wait_for(r2[c].at[0], send.at[A2, c, j])
            wait_for(r1[c].at[0], send.at[A3, c, j])
            wait_for(r0[c].at[j], send.at[FW, c, j])
            wait_for(r0[c].at[j], recv.at[FW, c, j])


def write_out(*refs):
    it = iter(refs)
    held = [[next(it) for _ in range(C)] for _ in range(2)]
    moments = [next(it) for _ in range(2 * C)]
    out = [next(it) for _ in range(C)]
    moments_out = [next(it) for _ in range(2 * C)]
    between = [next(it) for _ in range(2 * C)]
    sem, load, store = it
    core = lax.axis_index("dp") % 2

    for i in range(2 * C):
        pltpu.make_async_copy(moments[i], between[i], load.at[i]).start()

    @pl.loop(0, J)
    def _(j):
        for who in range(2):
            for c in range(C):
                for p in range(8):
                    blk = place(c, p // 4, p // 2 % 2, p % 2, core if who == 0 else 1 - core)
                    layer, rows, columns = part(c, j)
                    pltpu.make_async_copy(held[who][c].at[j, p], out[c].at[layer, blk, rows, columns], sem.at[who, c, j]).start()

    for i in range(2 * C):
        pltpu.make_async_copy(moments[i], between[i], load.at[i]).wait()
        pltpu.make_async_copy(between[i], moments_out[i], store.at[i]).start()

    @pl.loop(0, J)
    def _(j):
        for who in range(2):
            for c in range(C):
                pltpu.make_async_copy(held[who][c].at[j], held[who][c].at[j], sem.at[who, c, j]).wait()

    for i in range(2 * C):
        pltpu.make_async_copy(between[i], moments_out[i], store.at[i]).wait()


def solution(mesh):
    chunk = ((32, 8192 // SUB),) * 2 + ((512 // SUB, 512),)
    blocks = ((LAYERS, 16, 32, 8192),) * 2 + ((LAYERS, 16, 512, 512),)
    own = ((LAYERS, 32, 8192),) * 2 + ((LAYERS, 512, 512),)
    whole = ((LAYERS, 512, 8192),) * 2 + ((LAYERS, 8192, 512),)

    def vmem(*lead, dtype=BF16):
        return [pltpu.VMEM((*lead, *chunk[c]), dtype) for c in range(C)]

    anywhere, resident = pl.BlockSpec(memory_space=pl.ANY), pl.BlockSpec(memory_space=pltpu.VMEM)
    moments = [jax.ShapeDtypeStruct(s, F32) for s in own] * 2
    call = pl.pallas_call(
        kernel,
        out_shape=[*vmem(J, 8), *vmem(J, 8), *moments],
        in_specs=[anywhere] * 12,
        out_specs=[resident] * 6 + [anywhere] * 6,
        scratch_shapes=[
            *vmem(RING, 4),
            *vmem(RING, 2),
            *vmem(RING, 1),
            *vmem(2, 4),
            *vmem(2, 2),
            *vmem(2, 1),
            *vmem(2, 1),
            *vmem(2, dtype=F32),
            *vmem(2, dtype=F32),
            *vmem(2),
            pltpu.SemaphoreType.DMA((9, C, J)),
            pltpu.SemaphoreType.DMA((9, C, J)),
            pltpu.SemaphoreType.DMA((7, C, 2)),
            pltpu.SemaphoreType.DMA((2, C, 2)),
        ],
        compiler_params=pltpu.CompilerParams(collective_id=0, has_side_effects=True, vmem_limit_bytes=14 << 20),
    )
    finish = pl.pallas_call(
        write_out,
        out_shape=[jax.ShapeDtypeStruct(s, BF16) for s in blocks] + moments,
        in_specs=[resident] * 6 + [anywhere] * 6,
        out_specs=[anywhere] * 9,
        scratch_shapes=[
            *[pltpu.VMEM(s, F32) for s in own * 2],
            pltpu.SemaphoreType.DMA((2, C, J)),
            pltpu.SemaphoreType.DMA((2 * C,)),
            pltpu.SemaphoreType.DMA((2 * C,)),
        ],
        compiler_params=pltpu.CompilerParams(vmem_limit_bytes=14 << 20),
    )

    def step(*arrays):
        terms = [a.reshape(s) for a, s in zip(arrays[:3], blocks, strict=True)]
        weights = [a.reshape(s) for a, s in zip(arrays[3:6], blocks, strict=True)]
        kept = call(*terms, *weights, *arrays[6:])
        new = finish(*[pltpu.with_memory_space_constraint(a, pltpu.VMEM) for a in kept[:6]], *kept[6:])
        return (*(a.reshape(s) for a, s in zip(new[:3], whole, strict=True)), *new[3:])

    all_of, cut = P(None, None, None), P(None, "dp", None)
    return jax.shard_map(
        step,
        mesh=mesh,
        in_specs=(P(("rep", "dp"), None, None, None),) * 3 + (all_of,) * 3 + (cut,) * 6,
        out_specs=(P("rep", None, None),) * 3 + (P("rep", "dp", None),) * 6,
        check_vma=False,
    )
```

```python
import functools

import jax
import jax.numpy as jnp
from jax import lax
from jax.experimental import pallas as pl
from jax.experimental.pallas import tpu as pltpu
from jax.sharding import PartitionSpec as P

SUB = 8
LAYERS = 2
J = LAYERS * SUB
RING = 6
LATE, LATE_END = 8, 11
NX = LATE_END - LATE
AHEAD = 2
STRIDE = {"x": 8, "y": 4, "z": 2}
ORDER = (("x", "y", "z"), ("y", "z", "x"), ("z", "x", "y"))
C = 3
F32, BF16 = jnp.float32, jnp.bfloat16
MESH = pl.DeviceIdType.MESH
D0, DN, S1, S2, S3, A1, A2, A3, FW = range(9)


def adamw(w, m, v, g):
    m = 0.9 * m + 0.1 * g
    v = 0.95 * v + 0.05 * g * g
    step = m * lax.rsqrt(v + 1e-8) + 0.1 * w
    return (w - 0.02 * step).astype(BF16), m, v


def place(c, b0, b1, b2, k):
    s = [STRIDE[d] for d in ORDER[c]]
    return b0 * s[0] + b1 * s[1] + b2 * s[2] + k


def part(c, j):
    layer, s = j // SUB, j % SUB
    if c < 2:
        width = 8192 // SUB
        return layer, slice(None), pl.ds(pl.multiple_of(s * width, width), width)
    height = 512 // SUB
    return layer, pl.ds(pl.multiple_of(s * height, height), height), slice(None)


def is_late(j):
    return jnp.logical_and(j >= LATE, j < LATE_END)


def kernel(*refs):
    it = iter(refs)

    def take(n=C):
        return [next(it) for _ in range(n)]

    g, w, m, v = take(), take(), take(), take()
    r0, other, m_out, v_out, late = take(), take(), take(), take(), take()
    r1, r2, r3 = take(), take(), take()
    o1, o2, o3, o4 = take(), take(), take(), take()
    mb, vb, wb = take(), take(), take()
    send, recv, load, moved, kept = take(5)

    me = lax.axis_index("dp")
    core = me % 2
    bit = {d: me // s % 2 for d, s in STRIDE.items()}
    near = {d: me + s * (1 - 2 * bit[d]) for d, s in STRIDE.items()}
    partner = me + 1 - 2 * core
    mine = [tuple(bit[d] for d in ORDER[c]) for c in range(C)]

    def of_block(ref, c, blk, j):
        layer, rows, columns = part(c, j)
        return ref.at[layer, blk, rows, columns]

    def of_own(ref, c, j):
        layer, rows, columns = part(c, j)
        return ref.at[layer, rows, columns]

    def remote(c, j, group, src, dst, to):
        return pltpu.make_async_remote_copy(
            src_ref=src, dst_ref=dst, send_sem=send.at[group, c, j], recv_sem=recv.at[group, c, j], device_id={"dp": to}, device_id_type=MESH
        )

    def wait_for(ref, sem):
        pltpu.make_async_copy(ref, ref, sem).wait()

    def tiles(c, body, rows=32):
        if c < 2:
            across, down, high = 8192 // SUB // 512, 32 // rows, rows
        else:
            across, down = 1, 512 // SUB // rows

        @pl.loop(0, across * down)
        def _(i):
            row = pl.multiple_of(i % down * rows, rows)
            column = pl.multiple_of(i // down * 512, 512)
            body((pl.ds(row, rows), pl.ds(column, 512)))

    def start_exchange(j):
        for group in (D0, DN):
            for c in range(C):
                half = 1 - mine[c][0] if group == D0 else mine[c][0]
                for q in range(4):
                    blk = place(c, half, q // 2, q % 2, 1 - core)
                    remote(c, j, group, of_block(g[c], c, blk, j), r0[c].at[j, half * 4 + q], partner).start()

    def load_terms(stage, j):
        slot = j % 2
        for c in range(C):
            m0, m1, m2 = mine[c]
            if stage == 0:
                places = [(1 - m0, q // 2, q % 2) for q in range(4)]
            elif stage == 1:
                places = [(m0, 1 - m1, q) for q in range(2)]
            elif stage == 2:
                places = [(m0, m1, 1 - m2)]
            else:
                places = [(m0, m1, m2)]
            to = (o1, o2, o3, o4)[stage][c]
            for q, bits in enumerate(places):
                pltpu.make_async_copy(of_block(g[c], c, place(c, *bits, core), j), to.at[slot, q], load.at[stage, c, slot]).start()

    def load_own(j):
        slot = j % 2
        for c in range(C):

            @pl.when(j >= 2)
            def _():
                wait_for(mb[c].at[slot], moved.at[0, c, slot])
                wait_for(vb[c].at[slot], moved.at[1, c, slot])

            pltpu.make_async_copy(of_own(m[c], c, j), mb[c].at[slot], load.at[4, c, slot]).start()
            pltpu.make_async_copy(of_own(v[c], c, j), vb[c].at[slot], load.at[5, c, slot]).start()
            pltpu.make_async_copy(of_block(w[c], c, me, j), wb[c].at[slot], load.at[6, c, slot]).start()

    def stage1(j):
        slot = j % 2
        for c in range(C):
            m0, m1, m2 = mine[c]
            wait_for(r1[c].at[0], recv.at[D0, c, j])
            wait_for(o1[c].at[slot], load.at[0, c, slot])

            def body(at):
                for q in range(4):
                    p = (1 - m0) * 4 + q
                    r0[c][(j, p, *at)] = (r0[c][(j, p, *at)].astype(F32) + o1[c][(slot, q, *at)].astype(F32)).astype(BF16)

            tiles(c, body)
            remote(c, j, S1, r0[c].at[j, pl.ds((1 - m0) * 4, 4)], r1[c].at[j % RING], near[ORDER[c][0]]).start()

    def stage2(j):
        slot, ring = j % 2, j % RING
        for c in range(C):
            m0, m1, m2 = mine[c]
            wait_for(o2[c].at[slot], load.at[1, c, slot])
            wait_for(r1[c].at[0], recv.at[DN, c, j])
            wait_for(r1[c].at[0], recv.at[S1, c, j])
            wait_for(r1[c].at[0], send.at[S1, c, j])

            def body(at):
                for q in range(2):
                    p = (1 - m1) * 2 + q
                    total = r0[c][(j, m0 * 4 + p, *at)].astype(F32) + o2[c][(slot, q, *at)].astype(F32)
                    r1[c][(ring, p, *at)] = (total + r1[c][(ring, p, *at)].astype(F32)).astype(BF16)

            tiles(c, body)
            remote(c, j, S2, r1[c].at[ring, pl.ds((1 - m1) * 2, 2)], r2[c].at[ring], near[ORDER[c][1]]).start()

    def stage3(j):
        slot, ring = j % 2, j % RING
        for c in range(C):
            m0, m1, m2 = mine[c]
            wait_for(o3[c].at[slot], load.at[2, c, slot])
            wait_for(r2[c].at[0], recv.at[S2, c, j])
            wait_for(r2[c].at[0], send.at[S2, c, j])

            def body(at):
                p = 1 - m2
                total = r0[c][(j, m0 * 4 + m1 * 2 + p, *at)].astype(F32) + o3[c][(slot, 0, *at)].astype(F32)
                total = total + r1[c][(ring, m1 * 2 + p, *at)].astype(F32)
                r2[c][(ring, p, *at)] = (total + r2[c][(ring, p, *at)].astype(F32)).astype(BF16)

            tiles(c, body)
            remote(c, j, S3, r2[c].at[ring, pl.ds(1 - m2, 1)], r3[c].at[ring], near[ORDER[c][2]]).start()

    def give(c, j, p, n):
        remote(c, j, FW, r0[c].at[j, pl.ds(p, n)], other[c].at[j, pl.ds(p, n)], partner).start()

    def stage4(j):
        slot, ring = j % 2, j % RING
        for c in range(C):
            m0, m1, m2 = mine[c]
            here = m0 * 4 + m1 * 2 + m2
            wait_for(o4[c].at[slot], load.at[3, c, slot])
            wait_for(mb[c].at[slot], load.at[4, c, slot])
            wait_for(vb[c].at[slot], load.at[5, c, slot])
            wait_for(wb[c].at[slot], load.at[6, c, slot])
            wait_for(r3[c].at[0], recv.at[S3, c, j])
            wait_for(r3[c].at[0], send.at[S3, c, j])

            def body(at):
                total = r0[c][(j, here, *at)].astype(F32) + o4[c][(slot, 0, *at)].astype(F32)
                total = total + r1[c][(ring, m1 * 2 + m2, *at)].astype(F32)
                total = total + r2[c][(ring, m2, *at)].astype(F32)
                total = total + r3[c][(ring, 0, *at)].astype(F32)
                grad = total.astype(BF16).astype(F32)
                new = adamw(wb[c][(slot, *at)].astype(F32), mb[c][(slot, *at)], vb[c][(slot, *at)], grad)
                r0[c][(j, here, *at)], mb[c][(slot, *at)], vb[c][(slot, *at)] = new

            tiles(c, body, rows=16)
            remote(c, j, A1, r0[c].at[j, here], r0[c].at[j, here], near[ORDER[c][2]]).start()
            pltpu.make_async_copy(mb[c].at[slot], of_own(m_out[c], c, j), moved.at[0, c, slot]).start()
            pltpu.make_async_copy(vb[c].at[slot], of_own(v_out[c], c, j), moved.at[1, c, slot]).start()
            give(c, j, here, 1)

    def stage5(j):
        for c in range(C):
            m0, m1, m2 = mine[c]
            pair = m0 * 4 + m1 * 2
            wait_for(r3[c].at[0], recv.at[A1, c, j])
            remote(c, j, A2, r0[c].at[j, pl.ds(pair, 2)], r0[c].at[j, pl.ds(pair, 2)], near[ORDER[c][1]]).start()
            give(c, j, pair + 1 - m2, 1)

    def stage6(j):
        for c in range(C):
            m0, m1, m2 = mine[c]
            wait_for(r2[c].at[0], recv.at[A2, c, j])
            half = r0[c].at[j, pl.ds(m0 * 4, 4)]

            @pl.when(is_late(j))
            def _():
                pltpu.make_async_copy(half, late[c].at[j - LATE], kept.at[c, j - LATE]).start()

            @pl.when(jnp.logical_not(is_late(j)))
            def _():
                remote(c, j, A3, half, half, near[ORDER[c][0]]).start()

            give(c, j, m0 * 4 + (1 - m1) * 2, 2)

    def stage7(j):
        pl.when(jnp.logical_not(is_late(j)))(lambda: last_hop_in(j))

    def last_hop_in(j):
        for c in range(C):
            m0, m1, m2 = mine[c]
            wait_for(r1[c].at[0], recv.at[A3, c, j])
            give(c, j, (1 - m0) * 4, 4)

    def settle(j):
        for c in range(C):
            wait_for(r1[c].at[0], send.at[D0, c, j])
            wait_for(r1[c].at[0], send.at[DN, c, j])
            wait_for(r3[c].at[0], send.at[A1, c, j])
            wait_for(r2[c].at[0], send.at[A2, c, j])

            @pl.when(is_late(j))
            def _():
                wait_for(r1[c].at[0], kept.at[c, j - LATE])
                wait_for(r1[c].at[0], send.at[FW, c, j])
                wait_for(r1[c].at[0], recv.at[FW, c, j])

            @pl.when(jnp.logical_not(is_late(j)))
            def _():
                wait_for(r1[c].at[0], send.at[A3, c, j])
                wait_for(r0[c].at[j], send.at[FW, c, j])
                wait_for(r0[c].at[j], recv.at[FW, c, j])

    barrier = pltpu.get_barrier_semaphore()
    for to in (partner, *near.values()):
        pl.semaphore_signal(barrier, inc=1, device_id={"dp": to}, device_id_type=MESH)
    pl.semaphore_wait(barrier, 4)

    for j in range(AHEAD):
        start_exchange(j)
    load_terms(0, 0)

    @pl.loop(0, J + 6)
    def _(t):
        def on(j, run):
            pl.when(jnp.logical_and(j >= 0, j < J))(lambda: run(j))

        on(t + AHEAD, start_exchange)
        on(t + 1, functools.partial(load_terms, 0))
        on(t, functools.partial(load_terms, 1))
        on(t - 1, functools.partial(load_terms, 2))
        on(t - 2, functools.partial(load_terms, 3))
        on(t - 2, load_own)
        for back, stage in enumerate((stage1, stage2, stage3, stage4, stage5, stage6, stage7)):
            on(t - back, stage)
        on(t - 8, settle)

    for c in range(C):
        for slot in range(2):
            wait_for(mb[c].at[slot], moved.at[0, c, slot])
            wait_for(vb[c].at[slot], moved.at[1, c, slot])

    for j in range(J - 2, J):
        settle(j)


def write_weights(*refs):
    it = iter(refs)
    held = [[next(it) for _ in range(C)] for _ in range(2)]
    out = [next(it) for _ in range(C)]
    sem = next(it)
    me = lax.axis_index("dp")
    core = me % 2

    def each(j, run):
        for who in range(2):
            for c in range(C):
                near = me // STRIDE[ORDER[c][0]] % 2
                run(j, who, c, near, 0)
                pl.when(jnp.logical_not(is_late(j)))(functools.partial(run, j, who, c, 1 - near, 1))

    def begin(j, who, c, half, far):
        layer, rows, columns = part(c, j)
        for q in range(4):
            blk = place(c, half, q // 2, q % 2, core if who == 0 else 1 - core)
            source = held[who][c].at[j, half * 4 + q]
            pltpu.make_async_copy(source, out[c].at[layer, blk, rows, columns], sem.at[far, who, c, j]).start()

    def finish(j, who, c, half, far):
        some = held[who][c].at[j, pl.ds(0, 4)]
        pltpu.make_async_copy(some, some, sem.at[far, who, c, j]).wait()

    pl.loop(0, J)(lambda j: each(j, begin))
    pl.loop(0, J)(lambda j: each(j, finish))


def write_moments(*refs):
    it = iter(refs)
    moments, out, between = [[next(it) for _ in range(2 * C)] for _ in range(3)]
    load, store = it
    for i in range(2 * C):
        pltpu.make_async_copy(moments[i], between[i], load.at[i]).start()
    for i in range(2 * C):
        pltpu.make_async_copy(moments[i], between[i], load.at[i]).wait()
        pltpu.make_async_copy(between[i], out[i], store.at[i]).start()
    for i in range(2 * C):
        pltpu.make_async_copy(between[i], out[i], store.at[i]).wait()


def write_late(*refs):
    it = iter(refs)
    came = [[next(it) for _ in range(C)] for _ in range(2)]
    _ = [next(it) for _ in range(C)]
    out = [next(it) for _ in range(C)]
    sem = next(it)
    me = lax.axis_index("dp")
    core = me % 2
    for who in range(2):
        for c in range(C):
            far = 1 - me // STRIDE[ORDER[c][0]] % 2
            for i in range(NX):
                layer, rows, columns = part(c, LATE + i)
                for q in range(4):
                    blk = place(c, far, q // 2, q % 2, core if who == 0 else 1 - core)
                    pltpu.make_async_copy(came[who][c].at[i, q], out[c].at[layer, blk, rows, columns], sem.at[who, c]).start()
    for who in range(2):
        for c in range(C):
            pltpu.make_async_copy(came[who][c], came[who][c], sem.at[who, c]).wait()


def solution(mesh):
    chunk = ((32, 8192 // SUB),) * 2 + ((512 // SUB, 512),)
    blocks = ((LAYERS, 16, 32, 8192),) * 2 + ((LAYERS, 16, 512, 512),)
    own = ((LAYERS, 32, 8192),) * 2 + ((LAYERS, 512, 512),)
    whole = ((LAYERS, 512, 8192),) * 2 + ((LAYERS, 8192, 512),)

    def vmem(*lead, dtype=BF16):
        return [pltpu.VMEM((*lead, *chunk[c]), dtype) for c in range(C)]

    anywhere, resident = pl.BlockSpec(memory_space=pl.ANY), pl.BlockSpec(memory_space=pltpu.VMEM)
    moments = [jax.ShapeDtypeStruct(s, F32) for s in own] * 2
    call = pl.pallas_call(
        kernel,
        out_shape=[*vmem(J, 8), *vmem(J, 8), *moments, *(jax.ShapeDtypeStruct((NX, 4, *s), BF16) for s in chunk)],
        in_specs=[anywhere] * 12,
        out_specs=[resident] * 6 + [anywhere] * 9,
        scratch_shapes=[
            *vmem(RING, 4),
            *vmem(RING, 2),
            *vmem(RING, 1),
            *vmem(2, 4),
            *vmem(2, 2),
            *vmem(2, 1),
            *vmem(2, 1),
            *vmem(2, dtype=F32),
            *vmem(2, dtype=F32),
            *vmem(2),
            pltpu.SemaphoreType.DMA((9, C, J)),
            pltpu.SemaphoreType.DMA((9, C, J)),
            pltpu.SemaphoreType.DMA((7, C, 2)),
            pltpu.SemaphoreType.DMA((2, C, 2)),
            pltpu.SemaphoreType.DMA((C, NX)),
        ],
        compiler_params=pltpu.CompilerParams(collective_id=0, has_side_effects=True, vmem_limit_bytes=13 << 20),
    )
    weights_out = [jax.ShapeDtypeStruct(s, BF16) for s in blocks]

    def cost(us):
        return pl.CostEstimate(flops=int(us * 2e9), bytes_accessed=int(us * 3e6), transcendentals=0)

    put_weights = pl.pallas_call(
        write_weights,
        out_shape=weights_out,
        in_specs=[resident] * 6,
        out_specs=[anywhere] * 3,
        scratch_shapes=[pltpu.SemaphoreType.DMA((2, 2, C, J))],
        cost_estimate=cost(15),
        compiler_params=pltpu.CompilerParams(vmem_limit_bytes=13 << 20),
    )
    put_moments = pl.pallas_call(
        write_moments,
        out_shape=moments,
        in_specs=[anywhere] * 6,
        out_specs=[anywhere] * 6,
        scratch_shapes=[*[pltpu.VMEM(s, F32) for s in own * 2], pltpu.SemaphoreType.DMA((2 * C,)), pltpu.SemaphoreType.DMA((2 * C,))],
        cost_estimate=cost(8),
        compiler_params=pltpu.CompilerParams(vmem_limit_bytes=13 << 20),
    )
    last = pl.pallas_call(
        write_late,
        out_shape=weights_out,
        in_specs=[resident] * 6 + [anywhere] * 3,
        out_specs=[anywhere] * 3,
        scratch_shapes=[pltpu.SemaphoreType.DMA((2, C))],
        input_output_aliases={6: 0, 7: 1, 8: 2},
        compiler_params=pltpu.CompilerParams(vmem_limit_bytes=13 << 20),
    )

    def swap(a, stride):
        return lax.ppermute(a, "dp", [(i, i + stride * (1 - 2 * (i // stride % 2))) for i in range(16)])

    def step(*arrays):
        terms = [a.reshape(s) for a, s in zip(arrays[:3], blocks, strict=True)]
        weights = [a.reshape(s) for a, s in zip(arrays[3:6], blocks, strict=True)]
        kept = call(*terms, *weights, *arrays[6:])
        held = [pltpu.with_memory_space_constraint(a, pltpu.VMEM) for a in kept[:6]]
        came = [swap(kept[12 + c], STRIDE[ORDER[c][0]]) for c in range(C)]
        new = put_weights(*held)
        came, new, moved = lax.optimization_barrier((came, new, kept[6:12]))
        handed = [swap(a, 1) for a in came]
        moved = put_moments(*[pltpu.with_memory_space_constraint(a, pltpu.HBM) for a in moved])
        new = last(*[pltpu.with_memory_space_constraint(a, pltpu.VMEM) for a in (*came, *handed)], *new)
        return (*(a.reshape(s) for a, s in zip(new, whole, strict=True)), *moved)

    all_of, cut = P(None, None, None), P(None, "dp", None)
    return jax.shard_map(
        step,
        mesh=mesh,
        in_specs=(P(("rep", "dp"), None, None, None),) * 3 + (all_of,) * 3 + (cut,) * 6,
        out_specs=(P("rep", None, None),) * 3 + (P("rep", "dp", None),) * 6,
        check_vma=False,
    )
```

```python
import functools

import jax
import jax.numpy as jnp
from jax import lax
from jax.experimental import pallas as pl
from jax.experimental.pallas import tpu as pltpu
from jax.sharding import PartitionSpec as P

SUB = 8
LAYERS = 2
J = LAYERS * SUB
RING = 6
LATE, LATE_END = 12, 16
NX = LATE_END - LATE
AHEAD = 2
STRIDE = {"x": 8, "y": 4, "z": 2}
ORDER = (("x", "y", "z"), ("y", "z", "x"), ("z", "x", "y"))
C = 3
VMEM_LIMIT = 13500416
F32, BF16 = jnp.float32, jnp.bfloat16
MESH = pl.DeviceIdType.MESH
D0, DN, S1, S2, S3, A1, A2, A3, FW = range(9)


def adamw(w, m, v, g):
    m = 0.9 * m + 0.1 * g
    v = 0.95 * v + 0.05 * g * g
    step = m * lax.rsqrt(v + 1e-8) + 0.1 * w
    return (w - 0.02 * step).astype(BF16), m, v


def place(c, b0, b1, b2, k):
    s = [STRIDE[d] for d in ORDER[c]]
    return b0 * s[0] + b1 * s[1] + b2 * s[2] + k


def part(c, j):
    layer, s = j // SUB, j % SUB
    if c < 2:
        width = 8192 // SUB
        return layer, slice(None), pl.ds(pl.multiple_of(s * width, width), width)
    height = 512 // SUB
    return layer, pl.ds(pl.multiple_of(s * height, height), height), slice(None)


def is_late(j):
    return jnp.logical_and(j >= LATE, j < LATE_END)


def kernel(*refs):
    it = iter(refs)

    def take(n=C):
        return [next(it) for _ in range(n)]

    g, w, m, v = take(), take(), take(), take()
    r0, other, m_out, v_out, late = take(), take(), take(), take(), take()
    r1, r2, r3 = take(), take(), take()
    o1, o2, o3, o4 = take(), take(), take(), take()
    mb, vb, wb = take(), take(), take()
    send, recv, load, moved, kept = take(5)

    me = lax.axis_index("dp")
    core = me % 2
    bit = {d: me // s % 2 for d, s in STRIDE.items()}
    near = {d: me + s * (1 - 2 * bit[d]) for d, s in STRIDE.items()}
    partner = me + 1 - 2 * core
    mine = [tuple(bit[d] for d in ORDER[c]) for c in range(C)]

    def of_block(ref, c, blk, j):
        layer, rows, columns = part(c, j)
        return ref.at[layer, blk, rows, columns]

    def of_own(ref, c, j):
        layer, rows, columns = part(c, j)
        return ref.at[layer, rows, columns]

    def remote(c, j, group, src, dst, to):
        return pltpu.make_async_remote_copy(
            src_ref=src, dst_ref=dst, send_sem=send.at[group, c, j], recv_sem=recv.at[group, c, j], device_id={"dp": to}, device_id_type=MESH
        )

    def wait_for(ref, sem):
        pltpu.make_async_copy(ref, ref, sem).wait()

    def tiles(c, body, rows=32):
        if c < 2:
            across, down, high = 8192 // SUB // 512, 32 // rows, rows
        else:
            across, down = 1, 512 // SUB // rows

        @pl.loop(0, across * down)
        def _(i):
            row = pl.multiple_of(i % down * rows, rows)
            column = pl.multiple_of(i // down * 512, 512)
            body((pl.ds(row, rows), pl.ds(column, 512)))

    def start_exchange(j):
        for group in (D0, DN):
            for c in range(C):
                half = 1 - mine[c][0] if group == D0 else mine[c][0]
                for q in range(4):
                    blk = place(c, half, q // 2, q % 2, 1 - core)
                    remote(c, j, group, of_block(g[c], c, blk, j), r0[c].at[j, half * 4 + q], partner).start()

    def load_terms(stage, j):
        slot = j % 2
        for c in range(C):
            m0, m1, m2 = mine[c]
            if stage == 0:
                places = [(1 - m0, q // 2, q % 2) for q in range(4)]
            elif stage == 1:
                places = [(m0, 1 - m1, q) for q in range(2)]
            elif stage == 2:
                places = [(m0, m1, 1 - m2)]
            else:
                places = [(m0, m1, m2)]
            to = (o1, o2, o3, o4)[stage][c]
            for q, bits in enumerate(places):
                pltpu.make_async_copy(of_block(g[c], c, place(c, *bits, core), j), to.at[slot, q], load.at[stage, c, slot]).start()

    def load_own(j):
        slot = j % 2
        for c in range(C):

            @pl.when(j >= 2)
            def _():
                wait_for(mb[c].at[slot], moved.at[0, c, slot])
                wait_for(vb[c].at[slot], moved.at[1, c, slot])

            pltpu.make_async_copy(of_own(m[c], c, j), mb[c].at[slot], load.at[4, c, slot]).start()
            pltpu.make_async_copy(of_own(v[c], c, j), vb[c].at[slot], load.at[5, c, slot]).start()
            pltpu.make_async_copy(of_block(w[c], c, me, j), wb[c].at[slot], load.at[6, c, slot]).start()

    def stage1(j):
        slot = j % 2
        for c in range(C):
            m0, m1, m2 = mine[c]
            wait_for(r1[c].at[0], recv.at[D0, c, j])
            wait_for(o1[c].at[slot], load.at[0, c, slot])

            def body(at):
                for q in range(4):
                    p = (1 - m0) * 4 + q
                    r0[c][(j, p, *at)] = (r0[c][(j, p, *at)].astype(F32) + o1[c][(slot, q, *at)].astype(F32)).astype(BF16)

            tiles(c, body)
            remote(c, j, S1, r0[c].at[j, pl.ds((1 - m0) * 4, 4)], r1[c].at[j % RING], near[ORDER[c][0]]).start()

    def stage2(j):
        slot, ring = j % 2, j % RING
        for c in range(C):
            m0, m1, m2 = mine[c]
            wait_for(o2[c].at[slot], load.at[1, c, slot])
            wait_for(r1[c].at[0], recv.at[DN, c, j])
            wait_for(r1[c].at[0], recv.at[S1, c, j])
            wait_for(r1[c].at[0], send.at[S1, c, j])

            def body(at):
                for q in range(2):
                    p = (1 - m1) * 2 + q
                    total = r0[c][(j, m0 * 4 + p, *at)].astype(F32) + o2[c][(slot, q, *at)].astype(F32)
                    r1[c][(ring, p, *at)] = (total + r1[c][(ring, p, *at)].astype(F32)).astype(BF16)

            tiles(c, body)
            remote(c, j, S2, r1[c].at[ring, pl.ds((1 - m1) * 2, 2)], r2[c].at[ring], near[ORDER[c][1]]).start()

    def stage3(j):
        slot, ring = j % 2, j % RING
        for c in range(C):
            m0, m1, m2 = mine[c]
            wait_for(o3[c].at[slot], load.at[2, c, slot])
            wait_for(r2[c].at[0], recv.at[S2, c, j])
            wait_for(r2[c].at[0], send.at[S2, c, j])

            def body(at):
                p = 1 - m2
                total = r0[c][(j, m0 * 4 + m1 * 2 + p, *at)].astype(F32) + o3[c][(slot, 0, *at)].astype(F32)
                total = total + r1[c][(ring, m1 * 2 + p, *at)].astype(F32)
                r2[c][(ring, p, *at)] = (total + r2[c][(ring, p, *at)].astype(F32)).astype(BF16)

            tiles(c, body)
            remote(c, j, S3, r2[c].at[ring, pl.ds(1 - m2, 1)], r3[c].at[ring], near[ORDER[c][2]]).start()

    def give(c, j, p, n):
        remote(c, j, FW, r0[c].at[j, pl.ds(p, n)], other[c].at[j, pl.ds(p, n)], partner).start()

    def stage4(j):
        slot, ring = j % 2, j % RING
        for c in range(C):
            m0, m1, m2 = mine[c]
            here = m0 * 4 + m1 * 2 + m2
            wait_for(o4[c].at[slot], load.at[3, c, slot])
            wait_for(mb[c].at[slot], load.at[4, c, slot])
            wait_for(vb[c].at[slot], load.at[5, c, slot])
            wait_for(wb[c].at[slot], load.at[6, c, slot])
            wait_for(r3[c].at[0], recv.at[S3, c, j])
            wait_for(r3[c].at[0], send.at[S3, c, j])

            def body(at):
                total = r0[c][(j, here, *at)].astype(F32) + o4[c][(slot, 0, *at)].astype(F32)
                total = total + r1[c][(ring, m1 * 2 + m2, *at)].astype(F32)
                total = total + r2[c][(ring, m2, *at)].astype(F32)
                total = total + r3[c][(ring, 0, *at)].astype(F32)
                grad = total.astype(BF16).astype(F32)
                new = adamw(wb[c][(slot, *at)].astype(F32), mb[c][(slot, *at)], vb[c][(slot, *at)], grad)
                r0[c][(j, here, *at)], mb[c][(slot, *at)], vb[c][(slot, *at)] = new

            tiles(c, body, rows=16)
            remote(c, j, A1, r0[c].at[j, here], r0[c].at[j, here], near[ORDER[c][2]]).start()
            pltpu.make_async_copy(mb[c].at[slot], of_own(m_out[c], c, j), moved.at[0, c, slot]).start()
            pltpu.make_async_copy(vb[c].at[slot], of_own(v_out[c], c, j), moved.at[1, c, slot]).start()
            give(c, j, here, 1)

    def stage5(j):
        for c in range(C):
            m0, m1, m2 = mine[c]
            pair = m0 * 4 + m1 * 2
            wait_for(r3[c].at[0], recv.at[A1, c, j])
            remote(c, j, A2, r0[c].at[j, pl.ds(pair, 2)], r0[c].at[j, pl.ds(pair, 2)], near[ORDER[c][1]]).start()
            give(c, j, pair + 1 - m2, 1)

    def stage6(j):
        for c in range(C):
            m0, m1, m2 = mine[c]
            wait_for(r2[c].at[0], recv.at[A2, c, j])
            half = r0[c].at[j, pl.ds(m0 * 4, 4)]

            @pl.when(is_late(j))
            def _():
                pltpu.make_async_copy(half, late[c].at[j - LATE], kept.at[c, j - LATE]).start()

            @pl.when(jnp.logical_not(is_late(j)))
            def _():
                remote(c, j, A3, half, half, near[ORDER[c][0]]).start()

            give(c, j, m0 * 4 + (1 - m1) * 2, 2)

    def stage7(j):
        pl.when(jnp.logical_not(is_late(j)))(lambda: last_hop_in(j))

    def last_hop_in(j):
        for c in range(C):
            m0, m1, m2 = mine[c]
            wait_for(r1[c].at[0], recv.at[A3, c, j])
            give(c, j, (1 - m0) * 4, 4)

    def settle(j):
        for c in range(C):
            wait_for(r1[c].at[0], send.at[D0, c, j])
            wait_for(r1[c].at[0], send.at[DN, c, j])
            wait_for(r3[c].at[0], send.at[A1, c, j])
            wait_for(r2[c].at[0], send.at[A2, c, j])

            @pl.when(is_late(j))
            def _():
                wait_for(r1[c].at[0], kept.at[c, j - LATE])
                wait_for(r1[c].at[0], send.at[FW, c, j])
                wait_for(r1[c].at[0], recv.at[FW, c, j])

            @pl.when(jnp.logical_not(is_late(j)))
            def _():
                wait_for(r1[c].at[0], send.at[A3, c, j])
                wait_for(r0[c].at[j], send.at[FW, c, j])
                wait_for(r0[c].at[j], recv.at[FW, c, j])

    barrier = pltpu.get_barrier_semaphore()
    for to in (partner, *near.values()):
        pl.semaphore_signal(barrier, inc=1, device_id={"dp": to}, device_id_type=MESH)
    pl.semaphore_wait(barrier, 4)

    for j in range(AHEAD):
        start_exchange(j)
    load_terms(0, 0)

    @pl.loop(0, J + 6)
    def _(t):
        def on(j, run):
            pl.when(jnp.logical_and(j >= 0, j < J))(lambda: run(j))

        on(t + AHEAD, start_exchange)
        on(t + 1, functools.partial(load_terms, 0))
        on(t, functools.partial(load_terms, 1))
        on(t - 1, functools.partial(load_terms, 2))
        on(t - 2, functools.partial(load_terms, 3))
        on(t - 2, load_own)
        for back, stage in enumerate((stage1, stage2, stage3, stage4, stage5, stage6, stage7)):
            on(t - back, stage)
        on(t - 8, settle)

    for c in range(C):
        for slot in range(2):
            wait_for(mb[c].at[slot], moved.at[0, c, slot])
            wait_for(vb[c].at[slot], moved.at[1, c, slot])

    for j in range(J - 2, J):
        settle(j)


def write_results(*refs):
    it = iter(refs)
    held = [[next(it) for _ in range(C)] for _ in range(2)]
    moments = [next(it) for _ in range(2 * C)]
    out = [next(it) for _ in range(C)]
    moments_out = [next(it) for _ in range(2 * C)]
    between = [next(it) for _ in range(2 * C)]
    sem, load, store = it
    me = lax.axis_index("dp")
    core = me % 2

    def each(j, run):
        for who in range(2):
            for c in range(C):
                near = me // STRIDE[ORDER[c][0]] % 2
                run(j, who, c, near, 0)
                pl.when(jnp.logical_not(is_late(j)))(functools.partial(run, j, who, c, 1 - near, 1))

    def begin(j, who, c, half, far):
        layer, rows, columns = part(c, j)
        for q in range(4):
            blk = place(c, half, q // 2, q % 2, core if who == 0 else 1 - core)
            source = held[who][c].at[j, half * 4 + q]
            pltpu.make_async_copy(source, out[c].at[layer, blk, rows, columns], sem.at[far, who, c, j]).start()

    def finish(j, who, c, half, far):
        some = held[who][c].at[j, pl.ds(0, 4)]
        pltpu.make_async_copy(some, some, sem.at[far, who, c, j]).wait()

    for i in range(2 * C):
        pltpu.make_async_copy(moments[i], between[i], load.at[i]).start()
    pl.loop(0, J)(lambda j: each(j, begin))
    for i in range(2 * C):
        pltpu.make_async_copy(moments[i], between[i], load.at[i]).wait()
        pltpu.make_async_copy(between[i], moments_out[i], store.at[i]).start()
    pl.loop(0, J)(lambda j: each(j, finish))
    for i in range(2 * C):
        pltpu.make_async_copy(between[i], moments_out[i], store.at[i]).wait()


def write_late(own_core, *refs):
    it = iter(refs)
    came = [next(it) for _ in range(C)]
    _ = [next(it) for _ in range(C)]
    out = [next(it) for _ in range(C)]
    sem = next(it)
    me = lax.axis_index("dp")
    core = me % 2 if own_core else 1 - me % 2
    for c in range(C):
        far = 1 - me // STRIDE[ORDER[c][0]] % 2
        for i in range(NX):
            layer, rows, columns = part(c, LATE + i)
            for q in range(4):
                blk = place(c, far, q // 2, q % 2, core)
                pltpu.make_async_copy(came[c].at[i, q], out[c].at[layer, blk, rows, columns], sem.at[c]).start()
    for c in range(C):
        pltpu.make_async_copy(came[c], came[c], sem.at[c]).wait()


def solution(mesh):
    chunk = ((32, 8192 // SUB),) * 2 + ((512 // SUB, 512),)
    blocks = ((LAYERS, 16, 32, 8192),) * 2 + ((LAYERS, 16, 512, 512),)
    own = ((LAYERS, 32, 8192),) * 2 + ((LAYERS, 512, 512),)
    whole = ((LAYERS, 512, 8192),) * 2 + ((LAYERS, 8192, 512),)

    def vmem(*lead, dtype=BF16):
        return [pltpu.VMEM((*lead, *chunk[c]), dtype) for c in range(C)]

    anywhere, resident = pl.BlockSpec(memory_space=pl.ANY), pl.BlockSpec(memory_space=pltpu.VMEM)
    moments = [jax.ShapeDtypeStruct(s, F32) for s in own] * 2
    call = pl.pallas_call(
        kernel,
        out_shape=[*vmem(J, 8), *vmem(J, 8), *moments, *(jax.ShapeDtypeStruct((NX, 4, *s), BF16) for s in chunk)],
        in_specs=[anywhere] * 12,
        out_specs=[resident] * 6 + [anywhere] * 9,
        scratch_shapes=[
            *vmem(RING, 4),
            *vmem(RING, 2),
            *vmem(RING, 1),
            *vmem(2, 4),
            *vmem(2, 2),
            *vmem(2, 1),
            *vmem(2, 1),
            *vmem(2, dtype=F32),
            *vmem(2, dtype=F32),
            *vmem(2),
            pltpu.SemaphoreType.DMA((9, C, J)),
            pltpu.SemaphoreType.DMA((9, C, J)),
            pltpu.SemaphoreType.DMA((7, C, 2)),
            pltpu.SemaphoreType.DMA((2, C, 2)),
            pltpu.SemaphoreType.DMA((C, NX)),
        ],
        compiler_params=pltpu.CompilerParams(collective_id=0, has_side_effects=True, vmem_limit_bytes=VMEM_LIMIT),
    )
    weights_out = [jax.ShapeDtypeStruct(s, BF16) for s in blocks]

    def cost(us):
        return pl.CostEstimate(flops=int(us * 2e9), bytes_accessed=int(us * 3e6), transcendentals=0)

    put = pl.pallas_call(
        write_results,
        out_shape=weights_out + moments,
        in_specs=[resident] * 6 + [anywhere] * 6,
        out_specs=[anywhere] * 9,
        scratch_shapes=[
            *[pltpu.VMEM(s, F32) for s in own * 2],
            pltpu.SemaphoreType.DMA((2, 2, C, J)),
            pltpu.SemaphoreType.DMA((2 * C,)),
            pltpu.SemaphoreType.DMA((2 * C,)),
        ],
        cost_estimate=cost(23),
        compiler_params=pltpu.CompilerParams(vmem_limit_bytes=VMEM_LIMIT),
    )

    def put_late(own_core, came, new):
        return pl.pallas_call(
            functools.partial(write_late, own_core),
            out_shape=weights_out,
            in_specs=[resident] * 3 + [anywhere] * 3,
            out_specs=[anywhere] * 3,
            scratch_shapes=[pltpu.SemaphoreType.DMA((C,))],
            input_output_aliases={3: 0, 4: 1, 5: 2},
            cost_estimate=cost(5),
            compiler_params=pltpu.CompilerParams(vmem_limit_bytes=VMEM_LIMIT),
        )(*[pltpu.with_memory_space_constraint(a, pltpu.VMEM) for a in came], *new)

    def swap(a, stride):
        return lax.ppermute(a, "dp", [(i, i + stride * (1 - 2 * (i // stride % 2))) for i in range(16)])

    def step(*arrays):
        terms = [a.reshape(s) for a, s in zip(arrays[:3], blocks, strict=True)]
        weights = [a.reshape(s) for a, s in zip(arrays[3:6], blocks, strict=True)]
        kept = call(*terms, *weights, *arrays[6:])
        held = [pltpu.with_memory_space_constraint(a, pltpu.VMEM) for a in kept[:6]]
        came = [swap(kept[12 + c], STRIDE[ORDER[c][0]]) for c in range(C)]
        new = put(*held, *kept[6:12])
        came, new = lax.optimization_barrier((came, new))
        handed = [swap(a, 1) for a in came]
        put_there = put_late(True, came, new[:3])
        put_there = put_late(False, handed, put_there)
        return (*(a.reshape(s) for a, s in zip(put_there, whole, strict=True)), *new[3:])

    all_of, cut = P(None, None, None), P(None, "dp", None)
    return jax.shard_map(
        step,
        mesh=mesh,
        in_specs=(P(("rep", "dp"), None, None, None),) * 3 + (all_of,) * 3 + (cut,) * 6,
        out_specs=(P("rep", None, None),) * 3 + (P("rep", "dp", None),) * 6,
        check_vma=False,
    )
```

```python
import functools

import jax
import jax.numpy as jnp
from jax import lax
from jax.experimental import pallas as pl
from jax.experimental.pallas import tpu as pltpu
from jax.sharding import PartitionSpec as P

SUB = 8
LAYERS = 2
J = LAYERS * SUB
RING = 6
LATE, LATE_END = 12, 16
NX = LATE_END - LATE
AHEAD = 2
STRIDE = {"x": 8, "y": 4, "z": 2}
ORDER = (("x", "y", "z"), ("y", "z", "x"), ("z", "x", "y"))
C = 3
VMEM_LIMIT = 13500416
F32, BF16 = jnp.float32, jnp.bfloat16
MESH = pl.DeviceIdType.MESH
D0, DN, S1, S2, S3, A1, A2, A3, FW = range(9)


def adamw(w, m, v, g):
    m = 0.9 * m + 0.1 * g
    v = 0.95 * v + 0.05 * g * g
    step = m * lax.rsqrt(v + 1e-8) + 0.1 * w
    return (w - 0.02 * step).astype(BF16), m, v


def place(c, b0, b1, b2, k):
    s = [STRIDE[d] for d in ORDER[c]]
    return b0 * s[0] + b1 * s[1] + b2 * s[2] + k


def part(c, j):
    layer, s = j // SUB, j % SUB
    if c < 2:
        width = 8192 // SUB
        return layer, slice(None), pl.ds(pl.multiple_of(s * width, width), width)
    height = 512 // SUB
    return layer, pl.ds(pl.multiple_of(s * height, height), height), slice(None)


def is_late(j):
    return jnp.logical_and(j >= LATE, j < LATE_END)


def kernel(*refs):
    it = iter(refs)

    def take(n=C):
        return [next(it) for _ in range(n)]

    g, w, m, v = take(), take(), take(), take()
    r0, other, m_out, v_out, late = take(), take(), take(), take(), take()
    r1, r2, r3 = take(), take(), take()
    o1, o2, o3, o4 = take(), take(), take(), take()
    mb, vb, wb = take(), take(), take()
    send, recv, load, moved, kept = take(5)

    me = lax.axis_index("dp")
    core = me % 2
    bit = {d: me // s % 2 for d, s in STRIDE.items()}
    near = {d: me + s * (1 - 2 * bit[d]) for d, s in STRIDE.items()}
    partner = me + 1 - 2 * core
    mine = [tuple(bit[d] for d in ORDER[c]) for c in range(C)]

    def of_block(ref, c, blk, j):
        layer, rows, columns = part(c, j)
        return ref.at[layer, blk, rows, columns]

    def of_own(ref, c, j):
        layer, rows, columns = part(c, j)
        return ref.at[layer, rows, columns]

    def remote(c, j, group, src, dst, to):
        return pltpu.make_async_remote_copy(
            src_ref=src, dst_ref=dst, send_sem=send.at[group, c, j], recv_sem=recv.at[group, c, j], device_id={"dp": to}, device_id_type=MESH
        )

    def wait_for(ref, sem):
        pltpu.make_async_copy(ref, ref, sem).wait()

    def tiles(c, body, rows=32):
        if c < 2:
            across, down, high = 8192 // SUB // 512, 32 // rows, rows
        else:
            across, down = 1, 512 // SUB // rows

        @pl.loop(0, across * down)
        def _(i):
            row = pl.multiple_of(i % down * rows, rows)
            column = pl.multiple_of(i // down * 512, 512)
            body((pl.ds(row, rows), pl.ds(column, 512)))

    def start_exchange(j):
        for group in (D0, DN):
            for c in range(C):
                half = 1 - mine[c][0] if group == D0 else mine[c][0]
                for q in range(4):
                    blk = place(c, half, q // 2, q % 2, 1 - core)
                    remote(c, j, group, of_block(g[c], c, blk, j), r0[c].at[j, half * 4 + q], partner).start()

    def load_terms(stage, j):
        slot = j % 2
        for c in range(C):
            m0, m1, m2 = mine[c]
            if stage == 0:
                places = [(1 - m0, q // 2, q % 2) for q in range(4)]
            elif stage == 1:
                places = [(m0, 1 - m1, q) for q in range(2)]
            elif stage == 2:
                places = [(m0, m1, 1 - m2)]
            else:
                places = [(m0, m1, m2)]
            to = (o1, o2, o3, o4)[stage][c]
            for q, bits in enumerate(places):
                pltpu.make_async_copy(of_block(g[c], c, place(c, *bits, core), j), to.at[slot, q], load.at[stage, c, slot]).start()

    def load_own(j):
        slot = j % 2
        for c in range(C):

            @pl.when(j >= 2)
            def _():
                wait_for(mb[c].at[slot], moved.at[0, c, slot])
                wait_for(vb[c].at[slot], moved.at[1, c, slot])

            pltpu.make_async_copy(of_own(m[c], c, j), mb[c].at[slot], load.at[4, c, slot]).start()
            pltpu.make_async_copy(of_own(v[c], c, j), vb[c].at[slot], load.at[5, c, slot]).start()
            pltpu.make_async_copy(of_block(w[c], c, me, j), wb[c].at[slot], load.at[6, c, slot]).start()

    def stage1(j):
        slot = j % 2
        for c in range(C):
            m0, m1, m2 = mine[c]
            wait_for(r1[c].at[0], recv.at[D0, c, j])
            wait_for(o1[c].at[slot], load.at[0, c, slot])

            def body(at):
                for q in range(4):
                    p = (1 - m0) * 4 + q
                    r0[c][(j, p, *at)] = (r0[c][(j, p, *at)].astype(F32) + o1[c][(slot, q, *at)].astype(F32)).astype(BF16)

            tiles(c, body)
            remote(c, j, S1, r0[c].at[j, pl.ds((1 - m0) * 4, 4)], r1[c].at[j % RING], near[ORDER[c][0]]).start()

    def stage2(j):
        slot, ring = j % 2, j % RING
        for c in range(C):
            m0, m1, m2 = mine[c]
            wait_for(o2[c].at[slot], load.at[1, c, slot])
            wait_for(r1[c].at[0], recv.at[DN, c, j])
            wait_for(r1[c].at[0], recv.at[S1, c, j])
            wait_for(r1[c].at[0], send.at[S1, c, j])

            def body(at):
                for q in range(2):
                    p = (1 - m1) * 2 + q
                    total = r0[c][(j, m0 * 4 + p, *at)].astype(F32) + o2[c][(slot, q, *at)].astype(F32)
                    r1[c][(ring, p, *at)] = (total + r1[c][(ring, p, *at)].astype(F32)).astype(BF16)

            tiles(c, body)
            remote(c, j, S2, r1[c].at[ring, pl.ds((1 - m1) * 2, 2)], r2[c].at[ring], near[ORDER[c][1]]).start()

    def stage3(j):
        slot, ring = j % 2, j % RING
        for c in range(C):
            m0, m1, m2 = mine[c]
            wait_for(o3[c].at[slot], load.at[2, c, slot])
            wait_for(r2[c].at[0], recv.at[S2, c, j])
            wait_for(r2[c].at[0], send.at[S2, c, j])

            def body(at):
                p = 1 - m2
                total = r0[c][(j, m0 * 4 + m1 * 2 + p, *at)].astype(F32) + o3[c][(slot, 0, *at)].astype(F32)
                total = total + r1[c][(ring, m1 * 2 + p, *at)].astype(F32)
                r2[c][(ring, p, *at)] = (total + r2[c][(ring, p, *at)].astype(F32)).astype(BF16)

            tiles(c, body)
            remote(c, j, S3, r2[c].at[ring, pl.ds(1 - m2, 1)], r3[c].at[ring], near[ORDER[c][2]]).start()

    def give(c, j, p, n):
        remote(c, j, FW, r0[c].at[j, pl.ds(p, n)], other[c].at[j, pl.ds(p, n)], partner).start()

    def stage4(j):
        slot, ring = j % 2, j % RING
        for c in range(C):
            m0, m1, m2 = mine[c]
            here = m0 * 4 + m1 * 2 + m2
            wait_for(o4[c].at[slot], load.at[3, c, slot])
            wait_for(mb[c].at[slot], load.at[4, c, slot])
            wait_for(vb[c].at[slot], load.at[5, c, slot])
            wait_for(wb[c].at[slot], load.at[6, c, slot])
            wait_for(r3[c].at[0], recv.at[S3, c, j])
            wait_for(r3[c].at[0], send.at[S3, c, j])

            def body(at):
                total = r0[c][(j, here, *at)].astype(F32) + o4[c][(slot, 0, *at)].astype(F32)
                total = total + r1[c][(ring, m1 * 2 + m2, *at)].astype(F32)
                total = total + r2[c][(ring, m2, *at)].astype(F32)
                total = total + r3[c][(ring, 0, *at)].astype(F32)
                grad = total.astype(BF16).astype(F32)
                new = adamw(wb[c][(slot, *at)].astype(F32), mb[c][(slot, *at)], vb[c][(slot, *at)], grad)
                r0[c][(j, here, *at)], mb[c][(slot, *at)], vb[c][(slot, *at)] = new

            tiles(c, body, rows=16)
            remote(c, j, A1, r0[c].at[j, here], r0[c].at[j, here], near[ORDER[c][2]]).start()
            pltpu.make_async_copy(mb[c].at[slot], of_own(m_out[c], c, j), moved.at[0, c, slot]).start()
            pltpu.make_async_copy(vb[c].at[slot], of_own(v_out[c], c, j), moved.at[1, c, slot]).start()
            give(c, j, here, 1)

    def stage5(j):
        for c in range(C):
            m0, m1, m2 = mine[c]
            pair = m0 * 4 + m1 * 2
            wait_for(r3[c].at[0], recv.at[A1, c, j])
            remote(c, j, A2, r0[c].at[j, pl.ds(pair, 2)], r0[c].at[j, pl.ds(pair, 2)], near[ORDER[c][1]]).start()
            give(c, j, pair + 1 - m2, 1)

    def stage6(j):
        for c in range(C):
            m0, m1, m2 = mine[c]
            wait_for(r2[c].at[0], recv.at[A2, c, j])
            half = r0[c].at[j, pl.ds(m0 * 4, 4)]

            @pl.when(is_late(j))
            def _():
                pltpu.make_async_copy(half, late[c].at[j - LATE], kept.at[c, j - LATE]).start()

            @pl.when(jnp.logical_not(is_late(j)))
            def _():
                remote(c, j, A3, half, half, near[ORDER[c][0]]).start()

            give(c, j, m0 * 4 + (1 - m1) * 2, 2)

    def stage7(j):
        pl.when(jnp.logical_not(is_late(j)))(lambda: last_hop_in(j))

    def last_hop_in(j):
        for c in range(C):
            m0, m1, m2 = mine[c]
            wait_for(r1[c].at[0], recv.at[A3, c, j])
            give(c, j, (1 - m0) * 4, 4)

    def settle(j):
        for c in range(C):
            wait_for(r1[c].at[0], send.at[D0, c, j])
            wait_for(r1[c].at[0], send.at[DN, c, j])
            wait_for(r3[c].at[0], send.at[A1, c, j])
            wait_for(r2[c].at[0], send.at[A2, c, j])

            @pl.when(is_late(j))
            def _():
                wait_for(r1[c].at[0], kept.at[c, j - LATE])
                wait_for(r1[c].at[0], send.at[FW, c, j])
                wait_for(r1[c].at[0], recv.at[FW, c, j])

            @pl.when(jnp.logical_not(is_late(j)))
            def _():
                wait_for(r1[c].at[0], send.at[A3, c, j])
                wait_for(r0[c].at[j], send.at[FW, c, j])
                wait_for(r0[c].at[j], recv.at[FW, c, j])

    barrier = pltpu.get_barrier_semaphore()
    for to in (partner, *near.values()):
        pl.semaphore_signal(barrier, inc=1, device_id={"dp": to}, device_id_type=MESH)
    pl.semaphore_wait(barrier, 4)

    for j in range(AHEAD):
        start_exchange(j)
    load_terms(0, 0)

    @pl.loop(0, J + 6)
    def _(t):
        def on(j, run):
            pl.when(jnp.logical_and(j >= 0, j < J))(lambda: run(j))

        on(t + AHEAD, start_exchange)
        on(t + 1, functools.partial(load_terms, 0))
        on(t, functools.partial(load_terms, 1))
        on(t - 1, functools.partial(load_terms, 2))
        on(t - 2, functools.partial(load_terms, 3))
        on(t - 2, load_own)
        for back, stage in enumerate((stage1, stage2, stage3, stage4, stage5, stage6, stage7)):
            on(t - back, stage)
        on(t - 8, settle)

    for c in range(C):
        for slot in range(2):
            wait_for(mb[c].at[slot], moved.at[0, c, slot])
            wait_for(vb[c].at[slot], moved.at[1, c, slot])

    for j in range(J - 2, J):
        settle(j)


def write_results(*refs):
    it = iter(refs)
    held = [[next(it) for _ in range(C)] for _ in range(2)]
    moments = [next(it) for _ in range(2 * C)]
    out = [next(it) for _ in range(C)]
    moments_out = [next(it) for _ in range(2 * C)]
    between = [next(it) for _ in range(2 * C)]
    sem, load, store = it
    me = lax.axis_index("dp")
    core = me % 2

    def each(j, run):
        for who in range(2):
            for c in range(C):
                near = me // STRIDE[ORDER[c][0]] % 2
                run(j, who, c, near, 0)
                pl.when(jnp.logical_not(is_late(j)))(functools.partial(run, j, who, c, 1 - near, 1))

    def begin(j, who, c, half, far):
        layer, rows, columns = part(c, j)
        for q in range(4):
            blk = place(c, half, q // 2, q % 2, core if who == 0 else 1 - core)
            source = held[who][c].at[j, half * 4 + q]
            pltpu.make_async_copy(source, out[c].at[layer, blk, rows, columns], sem.at[far, who, c, j]).start()

    def finish(j, who, c, half, far):
        some = held[who][c].at[j, pl.ds(0, 4)]
        pltpu.make_async_copy(some, some, sem.at[far, who, c, j]).wait()

    for i in range(2 * C):
        pltpu.make_async_copy(moments[i], between[i], load.at[i]).start()
    pl.loop(0, J)(lambda j: each(j, begin))
    for i in range(2 * C):
        pltpu.make_async_copy(moments[i], between[i], load.at[i]).wait()
        pltpu.make_async_copy(between[i], moments_out[i], store.at[i]).start()
    pl.loop(0, J)(lambda j: each(j, finish))
    for i in range(2 * C):
        pltpu.make_async_copy(between[i], moments_out[i], store.at[i]).wait()


def write_late(c, own_core, came, _, out, sem):
    me = lax.axis_index("dp")
    core = me % 2 if own_core else 1 - me % 2
    far = 1 - me // STRIDE[ORDER[c][0]] % 2
    for i in range(NX):
        layer, rows, columns = part(c, LATE + i)
        for q in range(4):
            blk = place(c, far, q // 2, q % 2, core)
            pltpu.make_async_copy(came.at[i, q], out.at[layer, blk, rows, columns], sem).start()
    pltpu.make_async_copy(came, came, sem).wait()


def solution(mesh):
    chunk = ((32, 8192 // SUB),) * 2 + ((512 // SUB, 512),)
    blocks = ((LAYERS, 16, 32, 8192),) * 2 + ((LAYERS, 16, 512, 512),)
    own = ((LAYERS, 32, 8192),) * 2 + ((LAYERS, 512, 512),)
    whole = ((LAYERS, 512, 8192),) * 2 + ((LAYERS, 8192, 512),)

    def vmem(*lead, dtype=BF16):
        return [pltpu.VMEM((*lead, *chunk[c]), dtype) for c in range(C)]

    anywhere, resident = pl.BlockSpec(memory_space=pl.ANY), pl.BlockSpec(memory_space=pltpu.VMEM)
    moments = [jax.ShapeDtypeStruct(s, F32) for s in own] * 2
    call = pl.pallas_call(
        kernel,
        out_shape=[*vmem(J, 8), *vmem(J, 8), *moments, *(jax.ShapeDtypeStruct((NX, 4, *s), BF16) for s in chunk)],
        in_specs=[anywhere] * 12,
        out_specs=[resident] * 6 + [anywhere] * 9,
        scratch_shapes=[
            *vmem(RING, 4),
            *vmem(RING, 2),
            *vmem(RING, 1),
            *vmem(2, 4),
            *vmem(2, 2),
            *vmem(2, 1),
            *vmem(2, 1),
            *vmem(2, dtype=F32),
            *vmem(2, dtype=F32),
            *vmem(2),
            pltpu.SemaphoreType.DMA((9, C, J)),
            pltpu.SemaphoreType.DMA((9, C, J)),
            pltpu.SemaphoreType.DMA((7, C, 2)),
            pltpu.SemaphoreType.DMA((2, C, 2)),
            pltpu.SemaphoreType.DMA((C, NX)),
        ],
        compiler_params=pltpu.CompilerParams(collective_id=0, has_side_effects=True, vmem_limit_bytes=VMEM_LIMIT),
    )
    weights_out = [jax.ShapeDtypeStruct(s, BF16) for s in blocks]

    def cost(us):
        return pl.CostEstimate(flops=int(us * 2e9), bytes_accessed=int(us * 3e6), transcendentals=0)

    put = pl.pallas_call(
        write_results,
        out_shape=weights_out + moments,
        in_specs=[resident] * 6 + [anywhere] * 6,
        out_specs=[anywhere] * 9,
        scratch_shapes=[
            *[pltpu.VMEM(s, F32) for s in own * 2],
            pltpu.SemaphoreType.DMA((2, 2, C, J)),
            pltpu.SemaphoreType.DMA((2 * C,)),
            pltpu.SemaphoreType.DMA((2 * C,)),
        ],
        cost_estimate=cost(23),
        compiler_params=pltpu.CompilerParams(vmem_limit_bytes=VMEM_LIMIT),
    )

    def put_late(c, own_core, came, new):
        return pl.pallas_call(
            functools.partial(write_late, c, own_core),
            out_shape=weights_out[c],
            in_specs=[resident, anywhere],
            out_specs=anywhere,
            scratch_shapes=[pltpu.SemaphoreType.DMA],
            input_output_aliases={1: 0},
            cost_estimate=cost(2),
            compiler_params=pltpu.CompilerParams(vmem_limit_bytes=VMEM_LIMIT),
        )(pltpu.with_memory_space_constraint(came, pltpu.VMEM), new)

    def swap(a, stride):
        return lax.ppermute(a, "dp", [(i, i + stride * (1 - 2 * (i // stride % 2))) for i in range(16)])

    def step(*arrays):
        terms = [a.reshape(s) for a, s in zip(arrays[:3], blocks, strict=True)]
        weights = [a.reshape(s) for a, s in zip(arrays[3:6], blocks, strict=True)]
        kept = call(*terms, *weights, *arrays[6:])
        held = [pltpu.with_memory_space_constraint(a, pltpu.VMEM) for a in kept[:6]]
        came = [swap(kept[12 + c], STRIDE[ORDER[c][0]]) for c in range(C)]
        new = put(*held, *kept[6:12])
        came, new = lax.optimization_barrier((came, new))
        handed = [swap(a, 1) for a in came]
        put_there = [put_late(c, True, came[c], new[c]) for c in range(C)]
        put_there = [put_late(c, False, handed[c], put_there[c]) for c in range(C)]
        return (*(a.reshape(s) for a, s in zip(put_there, whole, strict=True)), *new[3:])

    all_of, cut = P(None, None, None), P(None, "dp", None)
    return jax.shard_map(
        step,
        mesh=mesh,
        in_specs=(P(("rep", "dp"), None, None, None),) * 3 + (all_of,) * 3 + (cut,) * 6,
        out_specs=(P("rep", None, None),) * 3 + (P("rep", "dp", None),) * 6,
        check_vma=False,
    )
```

```python
import functools

import jax
import jax.numpy as jnp
from jax import lax
from jax.experimental import pallas as pl
from jax.experimental.pallas import tpu as pltpu
from jax.sharding import PartitionSpec as P

SUB = 8
LAYERS = 2
J = LAYERS * SUB
RING = 6
LATE, LATE_END = 12, 16
NX = LATE_END - LATE
AHEAD = 2
STRIDE = {"x": 8, "y": 4, "z": 2}
ORDER = (("x", "y", "z"), ("y", "z", "x"), ("z", "x", "y"))
C = 3
VMEM_LIMIT = 13500416
F32, BF16 = jnp.float32, jnp.bfloat16
MESH = pl.DeviceIdType.MESH
D0, DN, S1, S2, S3, A1, A2, A3 = range(8)
SENT, CAME = 4, 8


def adamw(w, m, v, g):
    m = 0.9 * m + 0.1 * g
    v = 0.95 * v + 0.05 * g * g
    step = m * lax.rsqrt(v + 1e-8) + 0.1 * w
    return (w - 0.02 * step).astype(BF16), m, v


def place(c, b0, b1, b2, k):
    s = [STRIDE[d] for d in ORDER[c]]
    return b0 * s[0] + b1 * s[1] + b2 * s[2] + k


def part(c, j):
    layer, s = j // SUB, j % SUB
    if c < 2:
        width = 8192 // SUB
        return layer, slice(None), pl.ds(pl.multiple_of(s * width, width), width)
    height = 512 // SUB
    return layer, pl.ds(pl.multiple_of(s * height, height), height), slice(None)


def is_late(j):
    return jnp.logical_and(j >= LATE, j < LATE_END)


def kernel(*refs):
    it = iter(refs)

    def take(n=C):
        return [next(it) for _ in range(n)]

    g, w, m, v = take(), take(), take(), take()
    r0, other, m_out, v_out, late = take(), take(), take(), take(), take()
    r1, r2, r3 = take(), take(), take()
    o1, o2, o3, o4 = take(), take(), take(), take()
    mb, vb, wb = take(), take(), take()
    send, recv, forward, load, moved, kept = take(6)

    me = lax.axis_index("dp")
    core = me % 2
    bit = {d: me // s % 2 for d, s in STRIDE.items()}
    near = {d: me + s * (1 - 2 * bit[d]) for d, s in STRIDE.items()}
    partner = me + 1 - 2 * core
    mine = [tuple(bit[d] for d in ORDER[c]) for c in range(C)]

    def of_block(ref, c, blk, j):
        layer, rows, columns = part(c, j)
        return ref.at[layer, blk, rows, columns]

    def of_own(ref, c, j):
        layer, rows, columns = part(c, j)
        return ref.at[layer, rows, columns]

    def remote(c, j, group, src, dst, to):
        sems = dict(send_sem=send.at[group, c, j % SENT], recv_sem=recv.at[group, c, j % CAME])
        return pltpu.make_async_remote_copy(src_ref=src, dst_ref=dst, **sems, device_id={"dp": to}, device_id_type=MESH)

    def wait_for(ref, sem):
        pltpu.make_async_copy(ref, ref, sem).wait()

    def tiles(c, body, rows=32):
        if c < 2:
            across, down, high = 8192 // SUB // 512, 32 // rows, rows
        else:
            across, down = 1, 512 // SUB // rows

        @pl.loop(0, across * down)
        def _(i):
            row = pl.multiple_of(i % down * rows, rows)
            column = pl.multiple_of(i // down * 512, 512)
            body((pl.ds(row, rows), pl.ds(column, 512)))

    def start_exchange(j):
        for group in (D0, DN):
            for c in range(C):
                half = 1 - mine[c][0] if group == D0 else mine[c][0]
                for q in range(4):
                    blk = place(c, half, q // 2, q % 2, 1 - core)
                    remote(c, j, group, of_block(g[c], c, blk, j), r0[c].at[j, half * 4 + q], partner).start()

    def load_terms(stage, j):
        slot = j % 2
        for c in range(C):
            m0, m1, m2 = mine[c]
            if stage == 0:
                places = [(1 - m0, q // 2, q % 2) for q in range(4)]
            elif stage == 1:
                places = [(m0, 1 - m1, q) for q in range(2)]
            elif stage == 2:
                places = [(m0, m1, 1 - m2)]
            else:
                places = [(m0, m1, m2)]
            to = (o1, o2, o3, o4)[stage][c]
            for q, bits in enumerate(places):
                pltpu.make_async_copy(of_block(g[c], c, place(c, *bits, core), j), to.at[slot, q], load.at[stage, c, slot]).start()

    def load_own(j):
        slot = j % 2
        for c in range(C):

            @pl.when(j >= 2)
            def _():
                wait_for(mb[c].at[slot], moved.at[0, c, slot])
                wait_for(vb[c].at[slot], moved.at[1, c, slot])

            pltpu.make_async_copy(of_own(m[c], c, j), mb[c].at[slot], load.at[4, c, slot]).start()
            pltpu.make_async_copy(of_own(v[c], c, j), vb[c].at[slot], load.at[5, c, slot]).start()
            pltpu.make_async_copy(of_block(w[c], c, me, j), wb[c].at[slot], load.at[6, c, slot]).start()

    def stage1(j):
        slot = j % 2
        for c in range(C):
            m0, m1, m2 = mine[c]
            wait_for(r1[c].at[0], recv.at[D0, c, j % CAME])
            wait_for(o1[c].at[slot], load.at[0, c, slot])

            def body(at):
                for q in range(4):
                    p = (1 - m0) * 4 + q
                    r0[c][(j, p, *at)] = (r0[c][(j, p, *at)].astype(F32) + o1[c][(slot, q, *at)].astype(F32)).astype(BF16)

            tiles(c, body)
            remote(c, j, S1, r0[c].at[j, pl.ds((1 - m0) * 4, 4)], r1[c].at[j % RING], near[ORDER[c][0]]).start()

    def stage2(j):
        slot, ring = j % 2, j % RING
        for c in range(C):
            m0, m1, m2 = mine[c]
            wait_for(o2[c].at[slot], load.at[1, c, slot])
            wait_for(r1[c].at[0], recv.at[DN, c, j % CAME])
            wait_for(r1[c].at[0], send.at[D0, c, j % SENT])
            wait_for(r1[c].at[0], send.at[DN, c, j % SENT])
            wait_for(r1[c].at[0], recv.at[S1, c, j % CAME])
            wait_for(r1[c].at[0], send.at[S1, c, j % SENT])

            def body(at):
                for q in range(2):
                    p = (1 - m1) * 2 + q
                    total = r0[c][(j, m0 * 4 + p, *at)].astype(F32) + o2[c][(slot, q, *at)].astype(F32)
                    r1[c][(ring, p, *at)] = (total + r1[c][(ring, p, *at)].astype(F32)).astype(BF16)

            tiles(c, body)
            remote(c, j, S2, r1[c].at[ring, pl.ds((1 - m1) * 2, 2)], r2[c].at[ring], near[ORDER[c][1]]).start()

    def stage3(j):
        slot, ring = j % 2, j % RING
        for c in range(C):
            m0, m1, m2 = mine[c]
            wait_for(o3[c].at[slot], load.at[2, c, slot])
            wait_for(r2[c].at[0], recv.at[S2, c, j % CAME])
            wait_for(r2[c].at[0], send.at[S2, c, j % SENT])

            def body(at):
                p = 1 - m2
                total = r0[c][(j, m0 * 4 + m1 * 2 + p, *at)].astype(F32) + o3[c][(slot, 0, *at)].astype(F32)
                total = total + r1[c][(ring, m1 * 2 + p, *at)].astype(F32)
                r2[c][(ring, p, *at)] = (total + r2[c][(ring, p, *at)].astype(F32)).astype(BF16)

            tiles(c, body)
            remote(c, j, S3, r2[c].at[ring, pl.ds(1 - m2, 1)], r3[c].at[ring], near[ORDER[c][2]]).start()

    def give(c, j, p, n):
        sems = dict(send_sem=forward.at[0, c, j % CAME], recv_sem=forward.at[1, c, j % CAME])
        here, there = r0[c].at[j, pl.ds(p, n)], other[c].at[j, pl.ds(p, n)]
        pltpu.make_async_remote_copy(src_ref=here, dst_ref=there, **sems, device_id={"dp": partner}, device_id_type=MESH).start()

    def stage4(j):
        slot, ring = j % 2, j % RING
        for c in range(C):
            m0, m1, m2 = mine[c]
            here = m0 * 4 + m1 * 2 + m2
            wait_for(o4[c].at[slot], load.at[3, c, slot])
            wait_for(mb[c].at[slot], load.at[4, c, slot])
            wait_for(vb[c].at[slot], load.at[5, c, slot])
            wait_for(wb[c].at[slot], load.at[6, c, slot])
            wait_for(r3[c].at[0], recv.at[S3, c, j % CAME])
            wait_for(r3[c].at[0], send.at[S3, c, j % SENT])

            def body(at):
                total = r0[c][(j, here, *at)].astype(F32) + o4[c][(slot, 0, *at)].astype(F32)
                total = total + r1[c][(ring, m1 * 2 + m2, *at)].astype(F32)
                total = total + r2[c][(ring, m2, *at)].astype(F32)
                total = total + r3[c][(ring, 0, *at)].astype(F32)
                grad = total.astype(BF16).astype(F32)
                new = adamw(wb[c][(slot, *at)].astype(F32), mb[c][(slot, *at)], vb[c][(slot, *at)], grad)
                r0[c][(j, here, *at)], mb[c][(slot, *at)], vb[c][(slot, *at)] = new

            tiles(c, body, rows=16)
            remote(c, j, A1, r0[c].at[j, here], r0[c].at[j, here], near[ORDER[c][2]]).start()
            pltpu.make_async_copy(mb[c].at[slot], of_own(m_out[c], c, j), moved.at[0, c, slot]).start()
            pltpu.make_async_copy(vb[c].at[slot], of_own(v_out[c], c, j), moved.at[1, c, slot]).start()
            give(c, j, here, 1)

    def stage5(j):
        for c in range(C):
            m0, m1, m2 = mine[c]
            pair = m0 * 4 + m1 * 2
            wait_for(r3[c].at[0], recv.at[A1, c, j % CAME])
            remote(c, j, A2, r0[c].at[j, pl.ds(pair, 2)], r0[c].at[j, pl.ds(pair, 2)], near[ORDER[c][1]]).start()
            give(c, j, pair + 1 - m2, 1)

    def stage6(j):
        for c in range(C):
            m0, m1, m2 = mine[c]
            wait_for(r2[c].at[0], recv.at[A2, c, j % CAME])
            wait_for(r3[c].at[0], send.at[A1, c, j % SENT])
            wait_for(r2[c].at[0], send.at[A2, c, j % SENT])
            half = r0[c].at[j, pl.ds(m0 * 4, 4)]

            @pl.when(is_late(j))
            def _():
                pltpu.make_async_copy(half, late[c].at[j - LATE], kept.at[c, j - LATE]).start()

            @pl.when(jnp.logical_not(is_late(j)))
            def _():
                remote(c, j, A3, half, half, near[ORDER[c][0]]).start()

            give(c, j, m0 * 4 + (1 - m1) * 2, 2)

    def stage7(j):
        pl.when(jnp.logical_not(is_late(j)))(lambda: last_hop_in(j))

    def last_hop_in(j):
        for c in range(C):
            m0, m1, m2 = mine[c]
            wait_for(r1[c].at[0], recv.at[A3, c, j % CAME])
            wait_for(r1[c].at[0], send.at[A3, c, j % SENT])
            give(c, j, (1 - m0) * 4, 4)

    def settle(j):
        for c in range(C):

            @pl.when(is_late(j))
            def _():
                wait_for(r1[c].at[0], kept.at[c, j - LATE])
                wait_for(r1[c].at[0], forward.at[0, c, j % CAME])
                wait_for(r1[c].at[0], forward.at[1, c, j % CAME])

            @pl.when(jnp.logical_not(is_late(j)))
            def _():
                wait_for(r0[c].at[j], forward.at[0, c, j % CAME])
                wait_for(r0[c].at[j], forward.at[1, c, j % CAME])

    barrier = pltpu.get_barrier_semaphore()
    for to in (partner, *near.values()):
        pl.semaphore_signal(barrier, inc=1, device_id={"dp": to}, device_id_type=MESH)
    pl.semaphore_wait(barrier, 4)

    for j in range(AHEAD):
        start_exchange(j)
    load_terms(0, 0)

    @pl.loop(0, J + 6)
    def _(t):
        def on(j, run):
            pl.when(jnp.logical_and(j >= 0, j < J))(lambda: run(j))

        on(t + AHEAD, start_exchange)
        on(t + 1, functools.partial(load_terms, 0))
        on(t, functools.partial(load_terms, 1))
        on(t - 1, functools.partial(load_terms, 2))
        on(t - 2, functools.partial(load_terms, 3))
        on(t - 2, load_own)
        for back, stage in enumerate((stage1, stage2, stage3, stage4, stage5, stage6, stage7)):
            on(t - back, stage)
        on(t - 7, settle)

    for c in range(C):
        for slot in range(2):
            wait_for(mb[c].at[slot], moved.at[0, c, slot])
            wait_for(vb[c].at[slot], moved.at[1, c, slot])

    settle(J - 1)


def write_results(*refs):
    it = iter(refs)
    held = [[next(it) for _ in range(C)] for _ in range(2)]
    moments = [next(it) for _ in range(2 * C)]
    out = [next(it) for _ in range(C)]
    moments_out = [next(it) for _ in range(2 * C)]
    between = [next(it) for _ in range(2 * C)]
    sem, load, store = it
    me = lax.axis_index("dp")
    core = me % 2

    def each(j, run):
        for who in range(2):
            for c in range(C):
                near = me // STRIDE[ORDER[c][0]] % 2
                run(j, who, c, near, 0)
                pl.when(jnp.logical_not(is_late(j)))(functools.partial(run, j, who, c, 1 - near, 1))

    def begin(j, who, c, half, far):
        layer, rows, columns = part(c, j)
        for q in range(4):
            blk = place(c, half, q // 2, q % 2, core if who == 0 else 1 - core)
            source = held[who][c].at[j, half * 4 + q]
            pltpu.make_async_copy(source, out[c].at[layer, blk, rows, columns], sem.at[far, who, c]).start()

    for i in range(2 * C):
        pltpu.make_async_copy(moments[i], between[i], load.at[i]).start()
    pl.loop(0, J)(lambda j: each(j, begin))
    for i in range(2 * C):
        pltpu.make_async_copy(moments[i], between[i], load.at[i]).wait()
        pltpu.make_async_copy(between[i], moments_out[i], store.at[i]).start()
    for who in range(2):
        for c in range(C):
            for far, n in ((0, J), (1, LATE)):
                some = held[who][c].at[pl.ds(0, n), pl.ds(0, 4)]
                pltpu.make_async_copy(some, some, sem.at[far, who, c]).wait()
    for i in range(2 * C):
        pltpu.make_async_copy(between[i], moments_out[i], store.at[i]).wait()


def write_late(c, own_core, came, _, out, sem):
    me = lax.axis_index("dp")
    core = me % 2 if own_core else 1 - me % 2
    far = 1 - me // STRIDE[ORDER[c][0]] % 2
    for i in range(NX):
        layer, rows, columns = part(c, LATE + i)
        for q in range(4):
            blk = place(c, far, q // 2, q % 2, core)
            pltpu.make_async_copy(came.at[i, q], out.at[layer, blk, rows, columns], sem).start()
    pltpu.make_async_copy(came, came, sem).wait()


def solution(mesh):
    chunk = ((32, 8192 // SUB),) * 2 + ((512 // SUB, 512),)
    blocks = ((LAYERS, 16, 32, 8192),) * 2 + ((LAYERS, 16, 512, 512),)
    own = ((LAYERS, 32, 8192),) * 2 + ((LAYERS, 512, 512),)
    whole = ((LAYERS, 512, 8192),) * 2 + ((LAYERS, 8192, 512),)

    def vmem(*lead, dtype=BF16):
        return [pltpu.VMEM((*lead, *chunk[c]), dtype) for c in range(C)]

    anywhere, resident = pl.BlockSpec(memory_space=pl.ANY), pl.BlockSpec(memory_space=pltpu.VMEM)
    moments = [jax.ShapeDtypeStruct(s, F32) for s in own] * 2
    call = pl.pallas_call(
        kernel,
        out_shape=[*vmem(J, 8), *vmem(J, 8), *moments, *(jax.ShapeDtypeStruct((NX, 4, *s), BF16) for s in chunk)],
        in_specs=[anywhere] * 12,
        out_specs=[resident] * 6 + [anywhere] * 9,
        scratch_shapes=[
            *vmem(RING, 4),
            *vmem(RING, 2),
            *vmem(RING, 1),
            *vmem(2, 4),
            *vmem(2, 2),
            *vmem(2, 1),
            *vmem(2, 1),
            *vmem(2, dtype=F32),
            *vmem(2, dtype=F32),
            *vmem(2),
            pltpu.SemaphoreType.DMA((8, C, SENT)),
            pltpu.SemaphoreType.DMA((8, C, CAME)),
            pltpu.SemaphoreType.DMA((2, C, CAME)),
            pltpu.SemaphoreType.DMA((7, C, 2)),
            pltpu.SemaphoreType.DMA((2, C, 2)),
            pltpu.SemaphoreType.DMA((C, NX)),
        ],
        compiler_params=pltpu.CompilerParams(collective_id=0, has_side_effects=True, vmem_limit_bytes=VMEM_LIMIT),
    )
    weights_out = [jax.ShapeDtypeStruct(s, BF16) for s in blocks]

    def cost(us):
        return pl.CostEstimate(flops=int(us * 2e9), bytes_accessed=int(us * 3e6), transcendentals=0)

    put = pl.pallas_call(
        write_results,
        out_shape=weights_out + moments,
        in_specs=[resident] * 6 + [anywhere] * 6,
        out_specs=[anywhere] * 9,
        scratch_shapes=[
            *[pltpu.VMEM(s, F32) for s in own * 2],
            pltpu.SemaphoreType.DMA((2, 2, C)),
            pltpu.SemaphoreType.DMA((2 * C,)),
            pltpu.SemaphoreType.DMA((2 * C,)),
        ],
        cost_estimate=cost(23),
        compiler_params=pltpu.CompilerParams(vmem_limit_bytes=VMEM_LIMIT),
    )

    def put_late(c, own_core, came, new):
        return pl.pallas_call(
            functools.partial(write_late, c, own_core),
            out_shape=weights_out[c],
            in_specs=[resident, anywhere],
            out_specs=anywhere,
            scratch_shapes=[pltpu.SemaphoreType.DMA],
            input_output_aliases={1: 0},
            cost_estimate=cost(2),
            compiler_params=pltpu.CompilerParams(vmem_limit_bytes=VMEM_LIMIT),
        )(pltpu.with_memory_space_constraint(came, pltpu.VMEM), new)

    def swap(a, stride):
        return lax.ppermute(a, "dp", [(i, i + stride * (1 - 2 * (i // stride % 2))) for i in range(16)])

    def step(*arrays):
        terms = [a.reshape(s) for a, s in zip(arrays[:3], blocks, strict=True)]
        weights = [a.reshape(s) for a, s in zip(arrays[3:6], blocks, strict=True)]
        kept = call(*terms, *weights, *arrays[6:])
        held = [pltpu.with_memory_space_constraint(a, pltpu.VMEM) for a in kept[:6]]
        came = [swap(kept[12 + c], STRIDE[ORDER[c][0]]) for c in range(C)]
        new = put(*held, *kept[6:12])
        came, new = lax.optimization_barrier((came, new))
        handed = [swap(a, 1) for a in came]
        put_there = [put_late(c, True, came[c], new[c]) for c in range(C)]
        put_there = [put_late(c, False, handed[c], put_there[c]) for c in range(C)]
        return (*(a.reshape(s) for a, s in zip(put_there, whole, strict=True)), *new[3:])

    all_of, cut = P(None, None, None), P(None, "dp", None)
    return jax.shard_map(
        step,
        mesh=mesh,
        in_specs=(P(("rep", "dp"), None, None, None),) * 3 + (all_of,) * 3 + (cut,) * 6,
        out_specs=(P("rep", None, None),) * 3 + (P("rep", "dp", None),) * 6,
        check_vma=False,
    )
```

```python
import functools

import jax
import jax.numpy as jnp
from jax import lax
from jax.experimental import pallas as pl
from jax.experimental.pallas import tpu as pltpu
from jax.sharding import PartitionSpec as P

SUB = 8
LAYERS = 2
J = LAYERS * SUB
RING = 6
LATE, LATE_END = 12, 16
NX = LATE_END - LATE
AHEAD = 2
STRIDE = {"x": 8, "y": 4, "z": 2}
ORDER = (("x", "y", "z"), ("y", "z", "x"), ("z", "x", "y"))
C = 3
VMEM_LIMIT = 13500416
F32, BF16 = jnp.float32, jnp.bfloat16
MESH = pl.DeviceIdType.MESH
S1, S2, S3, A1, A2, A3, D0, DN = range(8)
SENT, CAME, LONG = 2, 4, 8


def adamw(w, m, v, g):
    m = 0.9 * m + 0.1 * g
    v = 0.95 * v + 0.05 * g * g
    step = m * lax.rsqrt(v + 1e-8) + 0.1 * w
    return (w - 0.02 * step).astype(BF16), m, v


def place(c, b0, b1, b2, k):
    s = [STRIDE[d] for d in ORDER[c]]
    return b0 * s[0] + b1 * s[1] + b2 * s[2] + k


def part(c, j):
    layer, s = j // SUB, j % SUB
    if c < 2:
        width = 8192 // SUB
        return layer, slice(None), pl.ds(pl.multiple_of(s * width, width), width)
    height = 512 // SUB
    return layer, pl.ds(pl.multiple_of(s * height, height), height), slice(None)


def is_late(j):
    return jnp.logical_and(j >= LATE, j < LATE_END)


def kernel(*refs):
    it = iter(refs)

    def take(n=C):
        return [next(it) for _ in range(n)]

    g, w, m, v = take(), take(), take(), take()
    r0, other, m_out, v_out, late = take(), take(), take(), take(), take()
    r1, r2, r3 = take(), take(), take()
    o1, o2, o3, o4 = take(), take(), take(), take()
    mb, vb, wb = take(), take(), take()
    send, recv, sent, came, forward, load, moved, kept = take(8)

    me = lax.axis_index("dp")
    core = me % 2
    bit = {d: me // s % 2 for d, s in STRIDE.items()}
    near = {d: me + s * (1 - 2 * bit[d]) for d, s in STRIDE.items()}
    partner = me + 1 - 2 * core
    mine = [tuple(bit[d] for d in ORDER[c]) for c in range(C)]

    def of_block(ref, c, blk, j):
        layer, rows, columns = part(c, j)
        return ref.at[layer, blk, rows, columns]

    def of_own(ref, c, j):
        layer, rows, columns = part(c, j)
        return ref.at[layer, rows, columns]

    def remote(c, j, group, src, dst, to):
        if group in (D0, DN):
            sems = dict(send_sem=sent.at[group - D0, c, j % CAME], recv_sem=came.at[group - D0, c, j % LONG])
        else:
            sems = dict(send_sem=send.at[group, c, j % SENT], recv_sem=recv.at[group, c, j % CAME])
        return pltpu.make_async_remote_copy(src_ref=src, dst_ref=dst, **sems, device_id={"dp": to}, device_id_type=MESH)

    def wait_for(ref, sem):
        pltpu.make_async_copy(ref, ref, sem).wait()

    def tiles(c, body, rows=32):
        if c < 2:
            across, down, high = 8192 // SUB // 512, 32 // rows, rows
        else:
            across, down = 1, 512 // SUB // rows

        @pl.loop(0, across * down)
        def _(i):
            row = pl.multiple_of(i % down * rows, rows)
            column = pl.multiple_of(i // down * 512, 512)
            body((pl.ds(row, rows), pl.ds(column, 512)))

    def start_exchange(j):
        for group in (D0, DN):
            for c in range(C):
                half = 1 - mine[c][0] if group == D0 else mine[c][0]
                for q in range(4):
                    blk = place(c, half, q // 2, q % 2, 1 - core)
                    remote(c, j, group, of_block(g[c], c, blk, j), r0[c].at[j, half * 4 + q], partner).start()

    def load_terms(stage, j):
        slot = j % 2
        for c in range(C):
            m0, m1, m2 = mine[c]
            if stage == 0:
                places = [(1 - m0, q // 2, q % 2) for q in range(4)]
            elif stage == 1:
                places = [(m0, 1 - m1, q) for q in range(2)]
            elif stage == 2:
                places = [(m0, m1, 1 - m2)]
            else:
                places = [(m0, m1, m2)]
            to = (o1, o2, o3, o4)[stage][c]
            for q, bits in enumerate(places):
                pltpu.make_async_copy(of_block(g[c], c, place(c, *bits, core), j), to.at[slot, q], load.at[stage, c, slot]).start()

    def load_own(j):
        slot = j % 2
        for c in range(C):

            @pl.when(j >= 2)
            def _():
                wait_for(mb[c].at[slot], moved.at[0, c, slot])
                wait_for(vb[c].at[slot], moved.at[1, c, slot])

            pltpu.make_async_copy(of_own(m[c], c, j), mb[c].at[slot], load.at[4, c, slot]).start()
            pltpu.make_async_copy(of_own(v[c], c, j), vb[c].at[slot], load.at[5, c, slot]).start()
            pltpu.make_async_copy(of_block(w[c], c, me, j), wb[c].at[slot], load.at[6, c, slot]).start()

    def stage1(j):
        slot = j % 2
        for c in range(C):
            m0, m1, m2 = mine[c]
            wait_for(r1[c].at[0], came.at[D0 - D0, c, j % LONG])
            wait_for(o1[c].at[slot], load.at[0, c, slot])

            def body(at):
                for q in range(4):
                    p = (1 - m0) * 4 + q
                    r0[c][(j, p, *at)] = (r0[c][(j, p, *at)].astype(F32) + o1[c][(slot, q, *at)].astype(F32)).astype(BF16)

            tiles(c, body)
            remote(c, j, S1, r0[c].at[j, pl.ds((1 - m0) * 4, 4)], r1[c].at[j % RING], near[ORDER[c][0]]).start()

    def stage2(j):
        slot, ring = j % 2, j % RING
        for c in range(C):
            m0, m1, m2 = mine[c]
            wait_for(o2[c].at[slot], load.at[1, c, slot])
            wait_for(r1[c].at[0], came.at[DN - D0, c, j % LONG])
            wait_for(r1[c].at[0], sent.at[D0 - D0, c, j % CAME])
            wait_for(r1[c].at[0], sent.at[DN - D0, c, j % CAME])
            wait_for(r1[c].at[0], recv.at[S1, c, j % CAME])
            wait_for(r1[c].at[0], send.at[S1, c, j % SENT])

            def body(at):
                for q in range(2):
                    p = (1 - m1) * 2 + q
                    total = r0[c][(j, m0 * 4 + p, *at)].astype(F32) + o2[c][(slot, q, *at)].astype(F32)
                    r1[c][(ring, p, *at)] = (total + r1[c][(ring, p, *at)].astype(F32)).astype(BF16)

            tiles(c, body)
            remote(c, j, S2, r1[c].at[ring, pl.ds((1 - m1) * 2, 2)], r2[c].at[ring], near[ORDER[c][1]]).start()

    def stage3(j):
        slot, ring = j % 2, j % RING
        for c in range(C):
            m0, m1, m2 = mine[c]
            wait_for(o3[c].at[slot], load.at[2, c, slot])
            wait_for(r2[c].at[0], recv.at[S2, c, j % CAME])
            wait_for(r2[c].at[0], send.at[S2, c, j % SENT])

            def body(at):
                p = 1 - m2
                total = r0[c][(j, m0 * 4 + m1 * 2 + p, *at)].astype(F32) + o3[c][(slot, 0, *at)].astype(F32)
                total = total + r1[c][(ring, m1 * 2 + p, *at)].astype(F32)
                r2[c][(ring, p, *at)] = (total + r2[c][(ring, p, *at)].astype(F32)).astype(BF16)

            tiles(c, body)
            remote(c, j, S3, r2[c].at[ring, pl.ds(1 - m2, 1)], r3[c].at[ring], near[ORDER[c][2]]).start()

    def give(c, j, p, n):
        sems = dict(send_sem=forward.at[0, c, j % LONG], recv_sem=forward.at[1, c, j % LONG])
        here, there = r0[c].at[j, pl.ds(p, n)], other[c].at[j, pl.ds(p, n)]
        pltpu.make_async_remote_copy(src_ref=here, dst_ref=there, **sems, device_id={"dp": partner}, device_id_type=MESH).start()

    def stage4(j):
        slot, ring = j % 2, j % RING
        for c in range(C):
            m0, m1, m2 = mine[c]
            here = m0 * 4 + m1 * 2 + m2
            wait_for(o4[c].at[slot], load.at[3, c, slot])
            wait_for(mb[c].at[slot], load.at[4, c, slot])
            wait_for(vb[c].at[slot], load.at[5, c, slot])
            wait_for(wb[c].at[slot], load.at[6, c, slot])
            wait_for(r3[c].at[0], recv.at[S3, c, j % CAME])
            wait_for(r3[c].at[0], send.at[S3, c, j % SENT])

            def body(at):
                total = r0[c][(j, here, *at)].astype(F32) + o4[c][(slot, 0, *at)].astype(F32)
                total = total + r1[c][(ring, m1 * 2 + m2, *at)].astype(F32)
                total = total + r2[c][(ring, m2, *at)].astype(F32)
                total = total + r3[c][(ring, 0, *at)].astype(F32)
                grad = total.astype(BF16).astype(F32)
                new = adamw(wb[c][(slot, *at)].astype(F32), mb[c][(slot, *at)], vb[c][(slot, *at)], grad)
                r0[c][(j, here, *at)], mb[c][(slot, *at)], vb[c][(slot, *at)] = new

            tiles(c, body, rows=16)
            remote(c, j, A1, r0[c].at[j, here], r0[c].at[j, here], near[ORDER[c][2]]).start()
            pltpu.make_async_copy(mb[c].at[slot], of_own(m_out[c], c, j), moved.at[0, c, slot]).start()
            pltpu.make_async_copy(vb[c].at[slot], of_own(v_out[c], c, j), moved.at[1, c, slot]).start()
            give(c, j, here, 1)

    def stage5(j):
        for c in range(C):
            m0, m1, m2 = mine[c]
            pair = m0 * 4 + m1 * 2
            wait_for(r3[c].at[0], recv.at[A1, c, j % CAME])
            wait_for(r3[c].at[0], send.at[A1, c, j % SENT])
            remote(c, j, A2, r0[c].at[j, pl.ds(pair, 2)], r0[c].at[j, pl.ds(pair, 2)], near[ORDER[c][1]]).start()
            give(c, j, pair + 1 - m2, 1)

    def stage6(j):
        for c in range(C):
            m0, m1, m2 = mine[c]
            wait_for(r2[c].at[0], recv.at[A2, c, j % CAME])
            wait_for(r2[c].at[0], send.at[A2, c, j % SENT])
            half = r0[c].at[j, pl.ds(m0 * 4, 4)]

            @pl.when(is_late(j))
            def _():
                pltpu.make_async_copy(half, late[c].at[j - LATE], kept.at[c, j - LATE]).start()

            @pl.when(jnp.logical_not(is_late(j)))
            def _():
                remote(c, j, A3, half, half, near[ORDER[c][0]]).start()

            give(c, j, m0 * 4 + (1 - m1) * 2, 2)

    def stage7(j):
        pl.when(jnp.logical_not(is_late(j)))(lambda: last_hop_in(j))

    def last_hop_in(j):
        for c in range(C):
            m0, m1, m2 = mine[c]
            wait_for(r1[c].at[0], recv.at[A3, c, j % CAME])
            wait_for(r1[c].at[0], send.at[A3, c, j % SENT])
            give(c, j, (1 - m0) * 4, 4)

    def settle(j):
        for c in range(C):

            @pl.when(is_late(j))
            def _():
                wait_for(r1[c].at[0], kept.at[c, j - LATE])
                wait_for(r1[c].at[0], forward.at[0, c, j % LONG])
                wait_for(r1[c].at[0], forward.at[1, c, j % LONG])

            @pl.when(jnp.logical_not(is_late(j)))
            def _():
                wait_for(r0[c].at[j], forward.at[0, c, j % LONG])
                wait_for(r0[c].at[j], forward.at[1, c, j % LONG])

    barrier = pltpu.get_barrier_semaphore()
    for to in (partner, *near.values()):
        pl.semaphore_signal(barrier, inc=1, device_id={"dp": to}, device_id_type=MESH)
    pl.semaphore_wait(barrier, 4)

    for j in range(AHEAD):
        start_exchange(j)
    load_terms(0, 0)

    @pl.loop(0, J + 6)
    def _(t):
        def on(j, run):
            pl.when(jnp.logical_and(j >= 0, j < J))(lambda: run(j))

        on(t + AHEAD, start_exchange)
        on(t + 1, functools.partial(load_terms, 0))
        on(t, functools.partial(load_terms, 1))
        on(t - 1, functools.partial(load_terms, 2))
        on(t - 2, functools.partial(load_terms, 3))
        on(t - 2, load_own)
        for back, stage in enumerate((stage1, stage2, stage3, stage4, stage5, stage6, stage7)):
            on(t - back, stage)
        on(t - 7, settle)

    for c in range(C):
        for slot in range(2):
            wait_for(mb[c].at[slot], moved.at[0, c, slot])
            wait_for(vb[c].at[slot], moved.at[1, c, slot])

    settle(J - 1)


def write_results(*refs):
    it = iter(refs)
    held = [[next(it) for _ in range(C)] for _ in range(2)]
    moments = [next(it) for _ in range(2 * C)]
    out = [next(it) for _ in range(C)]
    moments_out = [next(it) for _ in range(2 * C)]
    between = [next(it) for _ in range(2 * C)]
    sem, load, store = it
    me = lax.axis_index("dp")
    core = me % 2

    def each(j, run):
        for who in range(2):
            for c in range(C):
                near = me // STRIDE[ORDER[c][0]] % 2
                run(j, who, c, near, 0)
                pl.when(jnp.logical_not(is_late(j)))(functools.partial(run, j, who, c, 1 - near, 1))

    def begin(j, who, c, half, far):
        layer, rows, columns = part(c, j)
        for q in range(4):
            blk = place(c, half, q // 2, q % 2, core if who == 0 else 1 - core)
            source = held[who][c].at[j, half * 4 + q]
            pltpu.make_async_copy(source, out[c].at[layer, blk, rows, columns], sem.at[far, who, c]).start()

    for i in range(2 * C):
        pltpu.make_async_copy(moments[i], between[i], load.at[i]).start()
    pl.loop(0, J)(lambda j: each(j, begin))
    for i in range(2 * C):
        pltpu.make_async_copy(moments[i], between[i], load.at[i]).wait()
        pltpu.make_async_copy(between[i], moments_out[i], store.at[i]).start()
    for who in range(2):
        for c in range(C):
            for far, n in ((0, J), (1, LATE)):
                some = held[who][c].at[pl.ds(0, n), pl.ds(0, 4)]
                pltpu.make_async_copy(some, some, sem.at[far, who, c]).wait()
    for i in range(2 * C):
        pltpu.make_async_copy(between[i], moments_out[i], store.at[i]).wait()


def write_late(c, own_core, came, _, out, sem):
    me = lax.axis_index("dp")
    core = me % 2 if own_core else 1 - me % 2
    far = 1 - me // STRIDE[ORDER[c][0]] % 2
    for i in range(NX):
        layer, rows, columns = part(c, LATE + i)
        for q in range(4):
            blk = place(c, far, q // 2, q % 2, core)
            pltpu.make_async_copy(came.at[i, q], out.at[layer, blk, rows, columns], sem).start()
    pltpu.make_async_copy(came, came, sem).wait()


def solution(mesh):
    chunk = ((32, 8192 // SUB),) * 2 + ((512 // SUB, 512),)
    blocks = ((LAYERS, 16, 32, 8192),) * 2 + ((LAYERS, 16, 512, 512),)
    own = ((LAYERS, 32, 8192),) * 2 + ((LAYERS, 512, 512),)
    whole = ((LAYERS, 512, 8192),) * 2 + ((LAYERS, 8192, 512),)

    def vmem(*lead, dtype=BF16):
        return [pltpu.VMEM((*lead, *chunk[c]), dtype) for c in range(C)]

    anywhere, resident = pl.BlockSpec(memory_space=pl.ANY), pl.BlockSpec(memory_space=pltpu.VMEM)
    moments = [jax.ShapeDtypeStruct(s, F32) for s in own] * 2
    call = pl.pallas_call(
        kernel,
        out_shape=[*vmem(J, 8), *vmem(J, 8), *moments, *(jax.ShapeDtypeStruct((NX, 4, *s), BF16) for s in chunk)],
        in_specs=[anywhere] * 12,
        out_specs=[resident] * 6 + [anywhere] * 9,
        scratch_shapes=[
            *vmem(RING, 4),
            *vmem(RING, 2),
            *vmem(RING, 1),
            *vmem(2, 4),
            *vmem(2, 2),
            *vmem(2, 1),
            *vmem(2, 1),
            *vmem(2, dtype=F32),
            *vmem(2, dtype=F32),
            *vmem(2),
            pltpu.SemaphoreType.DMA((6, C, SENT)),
            pltpu.SemaphoreType.DMA((6, C, CAME)),
            pltpu.SemaphoreType.DMA((2, C, CAME)),
            pltpu.SemaphoreType.DMA((2, C, LONG)),
            pltpu.SemaphoreType.DMA((2, C, LONG)),
            pltpu.SemaphoreType.DMA((7, C, 2)),
            pltpu.SemaphoreType.DMA((2, C, 2)),
            pltpu.SemaphoreType.DMA((C, NX)),
        ],
        compiler_params=pltpu.CompilerParams(collective_id=0, has_side_effects=True, vmem_limit_bytes=VMEM_LIMIT),
    )
    weights_out = [jax.ShapeDtypeStruct(s, BF16) for s in blocks]

    def cost(us):
        return pl.CostEstimate(flops=int(us * 2e9), bytes_accessed=int(us * 3e6), transcendentals=0)

    put = pl.pallas_call(
        write_results,
        out_shape=weights_out + moments,
        in_specs=[resident] * 6 + [anywhere] * 6,
        out_specs=[anywhere] * 9,
        scratch_shapes=[
            *[pltpu.VMEM(s, F32) for s in own * 2],
            pltpu.SemaphoreType.DMA((2, 2, C)),
            pltpu.SemaphoreType.DMA((2 * C,)),
            pltpu.SemaphoreType.DMA((2 * C,)),
        ],
        cost_estimate=cost(23),
        compiler_params=pltpu.CompilerParams(vmem_limit_bytes=VMEM_LIMIT),
    )

    def put_late(c, own_core, came, new):
        return pl.pallas_call(
            functools.partial(write_late, c, own_core),
            out_shape=weights_out[c],
            in_specs=[resident, anywhere],
            out_specs=anywhere,
            scratch_shapes=[pltpu.SemaphoreType.DMA],
            input_output_aliases={1: 0},
            cost_estimate=cost(2),
            compiler_params=pltpu.CompilerParams(vmem_limit_bytes=VMEM_LIMIT),
        )(pltpu.with_memory_space_constraint(came, pltpu.VMEM), new)

    def swap(a, stride):
        return lax.ppermute(a, "dp", [(i, i + stride * (1 - 2 * (i // stride % 2))) for i in range(16)])

    def step(*arrays):
        terms = [a.reshape(s) for a, s in zip(arrays[:3], blocks, strict=True)]
        weights = [a.reshape(s) for a, s in zip(arrays[3:6], blocks, strict=True)]
        kept = call(*terms, *weights, *arrays[6:])
        held = [pltpu.with_memory_space_constraint(a, pltpu.VMEM) for a in kept[:6]]
        came = [swap(kept[12 + c], STRIDE[ORDER[c][0]]) for c in range(C)]
        new = put(*held, *kept[6:12])
        came, new = lax.optimization_barrier((came, new))
        handed = [swap(a, 1) for a in came]
        put_there = [put_late(c, True, came[c], new[c]) for c in range(C)]
        put_there = [put_late(c, False, handed[c], put_there[c]) for c in range(C)]
        return (*(a.reshape(s) for a, s in zip(put_there, whole, strict=True)), *new[3:])

    all_of, cut = P(None, None, None), P(None, "dp", None)
    return jax.shard_map(
        step,
        mesh=mesh,
        in_specs=(P(("rep", "dp"), None, None, None),) * 3 + (all_of,) * 3 + (cut,) * 6,
        out_specs=(P("rep", None, None),) * 3 + (P("rep", "dp", None),) * 6,
        check_vma=False,
    )
```
